128 devices in a mesh: row: 8 (over x, z_lo), col: 16 (over y, z_hi, core).
Axes of the slice: x: 4, y: 4, z: 4 (z_hi: 2, z_lo: 2; z = z_hi * 2 + z_lo), core: 2. Of those that a mesh axis runs over, the one named last changes fastest.
Arguments:
- cam_jac: bfloat16 [2, 2, 6, 2048, 1024], P(None, None, None, ('row', 'col')), may hold values from -0.09375 to 0.09375
- pt_jac: bfloat16 [2, 2, 3, 2048, 1024], P(None, None, None, ('row', 'col')), may hold values from -6 to 6
- resid: bfloat16 [2, 2, 2048, 1024], P(None, None, ('row', 'col')), may hold values from -6 to 6
- partner: int32 [2048, 1024], P(('row', 'col')), may hold values from 0 to 2047, as said below
- count: int32 [2048], P(('row', 'col')), may hold values from 512 to 1024
- tile_map: int32 [2048], replicated, may hold values from 0 to 2047, as said below
Outputs:
- coupling: bfloat16 [6, 6, 2048, 2048], P(None, None, 'row', 'col')
- camera_update: float32 [6, 2048], P(None, 'row')
- residual: float32 [6, 2048], P(None, 'row')
The draws below stay inside these ranges and needn't reach their ends.
Inputs may be any that keep to these rules, and one draw needn't show every extreme that they name: partner[a, t] is never a. `tile_map`: a permutation of the tile positions; of the 16 consecutive scenes of each device, exactly 2 have positions in each block of 256 consecutive positions.
All inputs are finite; a program needn't handle non-finite values.
Results may differ from the reference program's by a relative error of at most 0.0015.
Values may be sent and summed in bfloat16 or wider, within the bound.
A program may use at most 64 MiB of HBM per device.

```python
import jax
import jax.numpy as jnp
from jax import lax

SCN_DEV = 16
PTS = 1024
ITERS = 3
SCENES = 2048
TILE_ROWS = 256
PER_GROUP = 2


def draw_partner(key, part):
    scene_ids = jnp.arange(SCENES, dtype=jnp.int32)[:, None]
    offsets = jax.random.randint(key, (SCENES, PTS), 1, SCENES, dtype=jnp.int32)
    return ((scene_ids + offsets) % SCENES).astype(jnp.int32)


def draw_tile_map(key, part):
    devices = SCENES // SCN_DEV
    groups = SCENES // TILE_ROWS
    first_key, second_key = jax.random.split(jax.random.fold_in(key, 7))
    scores = jax.random.randint(first_key, (devices, SCN_DEV), 0, 1 << 14, dtype=jnp.int32) * SCN_DEV
    scores = scores + jnp.arange(SCN_DEV, dtype=jnp.int32)[None, :]
    local_rank = jnp.argsort(jnp.argsort(scores, axis=1), axis=1).astype(jnp.int32)
    group_of = local_rank // PER_GROUP
    within = jnp.arange(devices, dtype=jnp.int32)[:, None] * PER_GROUP + local_rank % PER_GROUP
    scores_two = jax.random.randint(second_key, (groups, TILE_ROWS), 0, 1 << 14, dtype=jnp.int32) * TILE_ROWS
    scores_two = scores_two + jnp.arange(TILE_ROWS, dtype=jnp.int32)[None, :]
    shuffle = jnp.argsort(jnp.argsort(scores_two, axis=1), axis=1).astype(jnp.int32)
    tiles = group_of * TILE_ROWS + shuffle[group_of, within]
    return tiles.reshape(SCENES).astype(jnp.int32)


def place_ends(values, own_key, least, top_value):
    longest = values.shape.index(max(values.shape))
    spots = []
    for shift in (0, 1):
        where = [jax.random.randint(jax.random.fold_in(own_key, axis), (), 0, length) for axis, length in enumerate(values.shape)]
        where[longest] = (where[longest] + shift) % values.shape[longest]
        spots.append(tuple(where))
    return values.at[spots[0]].set(least).at[spots[1]].set(top_value)


def steps_of(key, extent, pieces, least, top_value):
    factor_of, own = 1.0, jax.random.fold_in(key, 6)
    for position, parts in pieces:
        heights = jnp.exp(jax.random.uniform(jax.random.fold_in(own, position), (parts,), jnp.float32, least / len(pieces), top_value / len(pieces)))
        factor_of = factor_of * jnp.repeat(heights, extent[position] // parts).reshape([-1 if axis == position else 1 for axis in range(len(extent))])
    return factor_of


def bell_draw(key, shape, scale, most, pieces=(), held_as=jnp.bfloat16):
    entries = scale * jax.random.normal(key, shape, jnp.float32)
    if pieces:
        entries = entries * steps_of(key, shape, pieces, -0.22, 0.18)
    return jnp.clip(entries, -most, most).astype(held_as)


def setup_inputs(seed: int = 0) -> dict:
    key_of = jax.random.split(jax.random.key(seed), 7)
    cam_jac = bell_draw(key_of[0], (2, 2, 6, SCENES, PTS), (4 * PTS) ** -0.5, 0.09375, ((3, 128),))
    pt_jac = bell_draw(key_of[1], (2, 2, 3, SCENES, PTS), 1.0, 6.0, ((3, 128),))
    resid = bell_draw(key_of[2], (2, 2, SCENES, PTS), 1.0, 6.0, ((2, 128),))
    partner = draw_partner(jax.random.fold_in(key_of[6], 71), 0)
    count = place_ends(jax.random.randint(key_of[4], (SCENES,), PTS // 2, PTS + 1), jax.random.fold_in(key_of[4], 1), PTS // 2, PTS).astype(jnp.int32)
    tile_map = draw_tile_map(jax.random.fold_in(key_of[6], 71), 0)
    return dict(cam_jac=cam_jac, pt_jac=pt_jac, resid=resid, partner=partner, count=count, tile_map=tile_map)


CAMERA_DAMPING = 1.0
POINT_DAMPING = 1.0


def cross_product(first_vec, second_vec):
    return jnp.stack([first_vec[1] * second_vec[2] - first_vec[2] * second_vec[1],
                      first_vec[2] * second_vec[0] - first_vec[0] * second_vec[2],
                      first_vec[0] * second_vec[1] - first_vec[1] * second_vec[0]], axis=0)


def point_terms(camera, points_jac, errors):
    camera = camera.astype(jnp.float32)
    points_jac = points_jac.astype(jnp.float32)
    errors = errors.astype(jnp.float32)
    own_jac, other_jac = camera[0], camera[1]
    own_point, other_point = points_jac[0], points_jac[1]
    own_error, other_error = errors[0], errors[1]
    point_hessian = jnp.sum(own_point[:, :, None] * own_point[:, None, :], axis=0)
    point_hessian = point_hessian + jnp.sum(other_point[:, :, None] * other_point[:, None, :], axis=0)
    point_hessian = point_hessian + POINT_DAMPING * jnp.eye(3, dtype=jnp.float32)[:, :, None, None]
    first_row, second_row, third_row = point_hessian[0], point_hessian[1], point_hessian[2]
    cofactor_first = cross_product(second_row, third_row)
    cofactor_second = cross_product(third_row, first_row)
    cofactor_third = cross_product(first_row, second_row)
    determinant = jnp.sum(first_row * cofactor_first, axis=0)
    inverse = jnp.stack([cofactor_first, cofactor_second, cofactor_third], axis=1) / determinant
    w_own = jnp.sum(own_jac[:, :, None] * own_point[:, None, :], axis=0)
    w_other = jnp.sum(other_jac[:, :, None] * other_point[:, None, :], axis=0)
    point_rhs = -(jnp.sum(own_point * own_error[:, None], axis=0) + jnp.sum(other_point * other_error[:, None], axis=0))
    own_vi = jnp.sum(w_own[:, :, None] * inverse[None, :, :], axis=1)
    other_vi = jnp.sum(w_other[:, :, None] * inverse[None, :, :], axis=1)
    diag_own = jnp.sum(own_jac[:, :, None] * own_jac[:, None, :], axis=0) - jnp.sum(own_vi[:, None, :] * w_own[None, :, :], axis=2)
    diag_other = jnp.sum(other_jac[:, :, None] * other_jac[:, None, :], axis=0) - jnp.sum(other_vi[:, None, :] * w_other[None, :, :], axis=2)
    link = -jnp.sum(own_vi[:, None, :] * w_other[None, :, :], axis=2)
    grad_own = -jnp.sum(own_jac * own_error[:, None], axis=0) - jnp.sum(own_vi * point_rhs[None], axis=1)
    grad_other = -jnp.sum(other_jac * other_error[:, None], axis=0) - jnp.sum(other_vi * point_rhs[None], axis=1)
    return diag_own, diag_other, link, grad_own, grad_other


def reference(cam_jac, pt_jac, resid, partner, count, tile_map):
    blocks = SCENES // SCN_DEV

    def split_scenes(array):
        lead = array.shape[:-2]
        shaped = array.reshape(lead + (blocks, SCN_DEV, PTS))
        return jnp.moveaxis(shaped, len(lead), 0)

    inputs = (split_scenes(cam_jac), split_scenes(pt_jac), split_scenes(resid),
              partner.reshape(blocks, SCN_DEV, PTS), count.reshape(blocks, SCN_DEV),
              tile_map.reshape(blocks, SCN_DEV))

    def add_block(sums_so_far, block):
        coupling_flat, diag_sum, grad_sum = sums_so_far
        camera, points_jac, errors, partner_block, count_block, tile_block = block
        diag_own, diag_other, link, grad_own, grad_other = point_terms(camera, points_jac, errors)
        active = (jnp.arange(PTS, dtype=jnp.int32)[None, :] < count_block[:, None]).astype(jnp.float32)
        tile_other = jnp.take(tile_map, partner_block).astype(jnp.int32).reshape(-1)
        tile_own = jnp.broadcast_to(tile_block[:, None], (SCN_DEV, PTS)).astype(jnp.int32).reshape(-1)
        target = tile_own * SCENES + tile_other
        coupling_flat = coupling_flat.at[:, target].add((link * active).reshape(36, -1))
        diag_sum = diag_sum.at[:, tile_own].add((diag_own * active).reshape(36, -1))
        diag_sum = diag_sum.at[:, tile_other].add((diag_other * active).reshape(36, -1))
        grad_sum = grad_sum.at[:, tile_own].add((grad_own * active).reshape(6, -1))
        grad_sum = grad_sum.at[:, tile_other].add((grad_other * active).reshape(6, -1))
        return (coupling_flat, diag_sum, grad_sum), None

    start = (jnp.zeros((36, SCENES * SCENES), jnp.float32), jnp.zeros((36, SCENES), jnp.float32),
             jnp.zeros((6, SCENES), jnp.float32))
    (coupling_flat, diag_sum, grad_sum), unused = lax.scan(add_block, start, inputs)
    coupling = coupling_flat.reshape(6, 6, SCENES, SCENES).astype(jnp.bfloat16)
    coupling_wide = coupling.astype(jnp.float32)
    diag_blocks = diag_sum.reshape(6, 6, SCENES)

    def operator(vector):
        result = CAMERA_DAMPING * vector
        result = result + jnp.einsum('xyi,yi->xi', diag_blocks, vector, precision=lax.Precision.HIGHEST)
        result = result + jnp.einsum('xyij,yj->xi', coupling_wide, vector, precision=lax.Precision.HIGHEST)
        result = result + jnp.einsum('xyij,xi->yj', coupling_wide, vector, precision=lax.Precision.HIGHEST)
        return result

    solution = jnp.zeros((6, SCENES), jnp.float32)
    remainder = grad_sum
    direction = grad_sum
    norm_now = jnp.sum(remainder * remainder)
    for iteration in range(ITERS):
        product_vec = operator(direction)
        step_size = norm_now / jnp.sum(direction * product_vec)
        solution = solution + step_size * direction
        remainder = remainder - step_size * product_vec
        norm_next = jnp.sum(remainder * remainder)
        direction = remainder + (norm_next / norm_now) * direction
        norm_now = norm_next
    return coupling, solution, remainder
```

```python
import functools

import jax
import jax.numpy as jnp
from jax import lax
from jax.experimental import pallas as pl
from jax.experimental.pallas import tpu as pltpu
from jax.sharding import PartitionSpec as P

ITERS = 3
CAMERA_DAMPING = 1.0
POINT_DAMPING = 1.0

F32 = jnp.float32
BF16 = jnp.bfloat16
MESH = pl.DeviceIdType.MESH
LANES = 128

LINK = 36
PAIRS = [(x, y) for x in range(6) for y in range(x, 6)]
DIAG = len(PAIRS)
VALUES = 64
GRAD_AT = 24
SUM_ROWS = 32


def pair_index(x, y):
    return PAIRS.index((min(x, y), max(x, y)))


def dot3(first, second):
    total = first[0] * second[0]
    for k in range(1, len(first)):
        total = total + first[k] * second[k]
    return total


def point_chunk(cam_ref, pt_ref, res_ref, active, at):
    def cam(side, i):
        return [cam_ref[side, i, x, :, at].astype(F32) for x in range(6)]

    pa = [[pt_ref[0, i, k, :, at].astype(F32) for k in range(3)] for i in range(2)]
    pb = [[pt_ref[1, i, k, :, at].astype(F32) for k in range(3)] for i in range(2)]
    ea = [res_ref[0, i, :, at].astype(F32) for i in range(2)]
    eb = [res_ref[1, i, :, at].astype(F32) for i in range(2)]

    def hess(m, n):
        return pa[0][m] * pa[0][n] + pa[1][m] * pa[1][n] + (pb[0][m] * pb[0][n] + pb[1][m] * pb[1][n])

    v00, v11, v22 = (hess(k, k) + POINT_DAMPING for k in range(3))
    v01, v02, v12 = hess(0, 1), hess(0, 2), hess(1, 2)
    c00 = v11 * v22 - v12 * v12
    c01 = v02 * v12 - v01 * v22
    c02 = v01 * v12 - v02 * v11
    c11 = v00 * v22 - v02 * v02
    c12 = v01 * v02 - v00 * v12
    c22 = v00 * v11 - v01 * v01
    det = v00 * c00 + v01 * c01 + v02 * c02
    scale = 1.0 / det
    i00, i01, i02 = c00 * scale, c01 * scale, c02 * scale
    i11, i12, i22 = c11 * scale, c12 * scale, c22 * scale
    inv = [[i00, i01, i02], [i01, i11, i12], [i02, i12, i22]]
    q = [-(pa[0][k] * ea[0] + pa[1][k] * ea[1] + (pb[0][k] * eb[0] + pb[1][k] * eb[1])) for k in range(3)]
    pav = [[dot3(pa[i], inv[k]) for k in range(3)] for i in range(2)]
    pbv = [[dot3(pb[i], inv[k]) for k in range(3)] for i in range(2)]

    def schur(pv, p):
        n00 = (1.0 - dot3(pv[0], p[0])) * active
        n01 = -dot3(pv[0], p[1]) * active
        n11 = (1.0 - dot3(pv[1], p[1])) * active
        return [[n00, n01], [n01, n11]]

    naa, nbb = schur(pav, pa), schur(pbv, pb)
    mab = [[-dot3(pav[i], pb[j]) * active for j in range(2)] for i in range(2)]
    ga = [-(ea[i] + dot3(pav[i], q)) * active for i in range(2)]
    gb = [-(eb[i] + dot3(pbv[i], q)) * active for i in range(2)]
    ja = [cam(0, 0), cam(0, 1)]
    jb = [cam(1, 0), cam(1, 1)]

    def quad(left, middle, right, pairs):
        half = [[middle[i][0] * right[0][y] + middle[i][1] * right[1][y] for y in range(6)] for i in range(2)]
        return [left[0][x] * half[0][y] + left[1][x] * half[1][y] for x, y in pairs]

    link = quad(ja, mab, jb, [(x, y) for x in range(6) for y in range(6)])
    diag_other = quad(jb, nbb, jb, PAIRS)
    grad_other = [jb[0][x] * gb[0] + jb[1][x] * gb[1] for x in range(6)]
    diag_own = quad(ja, naa, ja, PAIRS)
    grad_own = [ja[0][x] * ga[0] + ja[1][x] * ga[1] for x in range(6)]
    return link + diag_other + grad_other, diag_own + grad_own


def assemble_kernel(
    own_ref, cam_ref, pt_ref, res_ref, partner_ref, count_ref, map_ref, own_col_ref,
    panel_ref, sums_ref,
    high, low, own_acc, lane_index, group_index, lhs, acc, weave, order,
):
    step = pl.program_id(0)
    scn, points = partner_ref.shape
    chunks = points // LANES
    scenes = map_ref.shape[0] * LANES
    groups = scenes // 256

    @pl.when(step == 0)
    def _():
        for s in range(scn):
            rank = jnp.int32(0)
            for t in range(scn):
                if t != s:
                    rank = rank + (own_ref[t] < own_ref[s]).astype(jnp.int32)
            order[rank] = jnp.int32(s)
        own_acc[...] = jnp.zeros_like(own_acc)
        acc[...] = jnp.zeros_like(acc)
        high[pl.ds((VALUES - 1) * scn, scn), :] = jnp.zeros((scn, points), F32)
        low[pl.ds((VALUES - 1) * scn, scn), :] = jnp.zeros((scn, points), F32)

        @pl.loop(0, chunks)
        def _(j):
            at = pl.ds(pl.multiple_of(j * LANES, LANES), LANES)
            slot = lax.broadcasted_iota(jnp.int32, (scn, LANES), 1) + j * LANES
            active = (slot < count_ref[...]).astype(F32)
            values, own = point_chunk(cam_ref, pt_ref, res_ref, active, at)
            for v, value in enumerate(values):
                top = value.astype(BF16).astype(F32)
                high[pl.ds(v * scn, scn), at] = top
                low[pl.ds(v * scn, scn), at] = value - top
            for v, value in enumerate(own):
                own_acc[v] += value
            partner = partner_ref[:, at]
            which = partner & (LANES - 1)
            line = partner >> 7
            tile = jnp.zeros((scn, LANES), jnp.int32)
            for h in range(map_ref.shape[0]):
                row = jnp.broadcast_to(map_ref[h : h + 1, :], (scn, LANES))
                tile = jnp.where(line == h, jnp.take_along_axis(row, which, axis=1), tile)
            column = tile >> 7
            lane_index[:, at] = ((column >> 3) << 7) | (tile & (LANES - 1))
            group_index[:, at] = column & 7

    for slot in range(2):
        s = order[step * 2 + slot]
        group_row = jnp.broadcast_to(group_index[pl.ds(s, 1), :], (groups, points))
        keep = group_row == lax.broadcasted_iota(jnp.int32, (groups, points), 0)
        lane_row = lane_index[pl.ds(s, 1), :]
        onehot = jnp.where(
            lane_row == lax.broadcasted_iota(jnp.int32, (256, points), 0), 1.0, 0.0
        ).astype(BF16)
        for part, source in enumerate((high, low)):
            for v in range(0, VALUES, 2):
                rows = [
                    jnp.where(keep, jnp.broadcast_to(source[pl.ds((v + k) * scn + s, 1), :], (groups, points)), 0.0)
                    for k in range(2)
                ]
                lhs[pl.ds((part * VALUES + v) * groups, 2 * groups), :] = jnp.concatenate(rows, axis=0).astype(BF16)
        result = lax.dot_general(
            lhs[...], onehot, (((1,), (1,)), ((), ())), preferred_element_type=F32
        )
        result = result[: VALUES * groups] + result[VALUES * groups :]
        for x in range(LINK):
            for b in range(2):
                weave[pl.ds((x * 2 + b) * 2 * groups + slot, groups, stride=2), :] = result[
                    x * groups : (x + 1) * groups, b * LANES : (b + 1) * LANES
                ]
        for b in range(2):
            acc[pl.ds(b * (VALUES - LINK) * groups, (VALUES - LINK) * groups), :] += result[
                LINK * groups :, b * LANES : (b + 1) * LANES
            ]
    panel_ref[...] = weave[...].reshape(LINK, 1, 2, 2 * groups, LANES).astype(BF16)

    @pl.when(step == pl.num_programs(0) - 1)
    def _():
        lanes = lax.broadcasted_iota(jnp.int32, (scn, LANES), 1)
        own_table = jnp.zeros((scn, LANES), F32)
        for v in range(DIAG + 6):
            total = jnp.sum(own_acc[v], axis=1, keepdims=True)
            own_table = jnp.where(lanes == (v if v < DIAG else GRAD_AT + v - DIAG), total, own_table)
        spread = (own_col_ref[...] == lax.broadcasted_iota(jnp.int32, (scn, scenes), 1)).astype(F32)
        own_sum = lax.dot_general(
            own_table.T[:SUM_ROWS], spread, (((1,), (0,)), ((), ())),
            precision=lax.Precision.HIGHEST, preferred_element_type=F32,
        )
        zeros = jnp.zeros((3, LANES), F32)
        for b in range(2):
            for h in range(groups):
                column = b * groups + h
                other = acc[pl.ds(b * (VALUES - LINK) * groups + h, VALUES - LINK, stride=groups), :]
                whole = jnp.concatenate(
                    [other[:DIAG], zeros, other[DIAG : DIAG + 6], zeros[:2]], axis=0
                )
                sums_ref[column // 2, :, (column % 2) * LANES : (column % 2 + 1) * LANES] = (
                    whole + own_sum[:, column * LANES : (column + 1) * LANES]
                )


def assemble(cam_jac, pt_jac, resid, partner, count, tile_map, tile_own):
    scn, points = partner.shape
    scenes = tile_map.shape[0]
    groups = scenes // 256
    rows = scenes // 256
    whole = lambda shape: pl.BlockSpec(shape, lambda i: (0,) * len(shape))
    map2 = tile_map.reshape(scenes // LANES, LANES)
    return pl.pallas_call(
        assemble_kernel,
        grid=(rows,),
        in_specs=[
            pl.BlockSpec(memory_space=pltpu.SMEM),
            whole(cam_jac.shape),
            whole(pt_jac.shape),
            whole(resid.shape),
            whole(partner.shape),
            whole((scn, 1)),
            whole(map2.shape),
            whole((scn, 1)),
        ],
        out_specs=[
            pl.BlockSpec((LINK, 1, 2, 2 * groups, LANES), lambda i: (0, i, 0, 0, 0)),
            whole((rows, SUM_ROWS, 256)),
        ],
        out_shape=[
            jax.ShapeDtypeStruct((LINK, rows, 2, 2 * groups, LANES), BF16),
            jax.ShapeDtypeStruct((rows, SUM_ROWS, 256), F32),
        ],
        scratch_shapes=[
            pltpu.VMEM((VALUES * scn, points), F32),
            pltpu.VMEM((VALUES * scn, points), F32),
            pltpu.VMEM((DIAG + 6, scn, LANES), F32),
            pltpu.VMEM((scn, points), jnp.int32),
            pltpu.VMEM((scn, points), jnp.int32),
            pltpu.VMEM((2 * VALUES * groups, points), BF16),
            pltpu.VMEM((2 * (VALUES - LINK) * groups, LANES), F32),
            pltpu.VMEM((LINK * 2 * 2 * groups, LANES), F32),
            pltpu.SMEM((scn,), jnp.int32),
        ],
        compiler_params=pltpu.CompilerParams(
            dimension_semantics=("arbitrary",), vmem_limit_bytes=48 * 1024 * 1024
        ),
        name="assemble",
    )(tile_own, cam_jac, pt_jac, resid, partner, count.reshape(scn, 1), map2, tile_own.reshape(scn, 1))


def select_kernel(tiles_ref, received_ref, out_ref, selection):
    row_start = lax.axis_index("row") * 256

    @pl.when(pl.program_id(0) == 0)
    def _():
        offset = tiles_ref[...] - row_start
        inside = (offset >= 0) & (offset < 256)
        least = jnp.min(jnp.where(inside, offset, 256), axis=0, keepdims=True)
        most = jnp.max(jnp.where(inside, offset, -1), axis=0, keepdims=True)
        odd = lax.broadcasted_iota(jnp.int32, least.shape, 1) & 1
        position = jnp.where(odd == 0, least, most)
        slots = position.shape[1]
        selection[...] = jnp.where(
            position == lax.broadcasted_iota(jnp.int32, (256, slots), 0), 1.0, 0.0
        ).astype(BF16)

    for k in range(received_ref.shape[0]):
        out_ref[k] = jnp.dot(selection[...], received_ref[k], preferred_element_type=F32).astype(BF16)


def select_rows(tile_map, received, scn):
    devices = tile_map.shape[0] // scn
    tiles = jnp.repeat(tile_map.reshape(devices, scn).T, 2, axis=1)
    block = 6
    return pl.pallas_call(
        select_kernel,
        grid=(LINK // block,),
        in_specs=[
            pl.BlockSpec(tiles.shape, lambda i: (0, 0)),
            pl.BlockSpec((block, 256, LANES), lambda i: (i, 0, 0)),
        ],
        out_specs=pl.BlockSpec((block, 256, LANES), lambda i: (i, 0, 0)),
        out_shape=jax.ShapeDtypeStruct((LINK, 256, LANES), BF16),
        scratch_shapes=[pltpu.VMEM((256, 2 * devices), BF16)],
        compiler_params=pltpu.CompilerParams(dimension_semantics=("arbitrary",)),
        name="select_rows",
    )(tiles, received)


def spread_along(axis, n, buffer, send, recv):
    me = lax.axis_index(axis)
    copies = []
    for k in range(1, n):
        there = lax.rem(me + k, n)
        copy = pltpu.make_async_remote_copy(
            src_ref=buffer.at[me],
            dst_ref=buffer.at[me],
            send_sem=send.at[k],
            recv_sem=recv.at[k],
            device_id={axis: there},
            device_id_type=MESH,
        )
        copy.start()
        copies.append(copy)
    return copies


def enter(rows, cols):
    barrier = pltpu.get_barrier_semaphore()
    for axis, n in (("row", rows), ("col", cols)):
        me = lax.axis_index(axis)
        for k in range(1, n):
            pl.semaphore_signal(barrier, inc=1, device_id={axis: lax.rem(me + k, n)}, device_id_type=MESH)
    pl.semaphore_wait(barrier, rows + cols - 2)


def slot_sum(buffer):
    total = buffer[0]
    for k in range(1, buffer.shape[0]):
        total = total + buffer[k]
    return total


def diagonal_kernel(
    rows, cols, sums_ref, blocks_ref, right_ref, parts, first, second,
    send_parts, recv_parts, send_first, recv_first, send_second, recv_second,
):
    row, col = lax.axis_index("row"), lax.axis_index("col")
    enter(rows, cols)
    copies = []
    for k in range(1, rows):
        there = lax.rem(row + k, rows)
        copy = pltpu.make_async_remote_copy(
            src_ref=sums_ref.at[there],
            dst_ref=parts.at[row],
            send_sem=send_parts.at[k],
            recv_sem=recv_parts.at[k],
            device_id={"row": there},
            device_id_type=MESH,
        )
        copy.start()
        copies.append(copy)
    parts[row] = sums_ref[row]
    for copy in copies:
        copy.wait()
    total = slot_sum(parts)
    first[col] = total[GRAD_AT : GRAD_AT + 8]
    copies = spread_along("col", cols, first, send_first, recv_first)
    line = lax.broadcasted_iota(jnp.int32, (8, 256), 0)
    for y in range(6):
        block = jnp.zeros((8, 256), F32)
        for x in range(6):
            v = pair_index(x, y)
            block = jnp.where(line == x, jnp.broadcast_to(total[v : v + 1], (8, 256)), block)
        blocks_ref[y] = block
    for copy in copies:
        copy.wait()
    second[row] = slot_sum(first)
    for copy in spread_along("row", rows, second, send_second, recv_second):
        copy.wait()
    right_ref[...] = second[...]


def add_diagonals(sums, rows, cols):
    return pl.pallas_call(
        functools.partial(diagonal_kernel, rows, cols),
        in_specs=[pl.BlockSpec(memory_space=pltpu.VMEM)],
        out_specs=[pl.BlockSpec(memory_space=pltpu.VMEM)] * 2,
        out_shape=[
            jax.ShapeDtypeStruct((6, 8, 256), F32),
            jax.ShapeDtypeStruct((rows, 8, 256), F32),
        ],
        scratch_shapes=[
            pltpu.VMEM((rows, SUM_ROWS, 256), F32),
            pltpu.VMEM((cols, 8, 256), F32),
            pltpu.VMEM((rows, 8, 256), F32),
            pltpu.SemaphoreType.DMA((rows,)),
            pltpu.SemaphoreType.DMA((rows,)),
            pltpu.SemaphoreType.DMA((cols,)),
            pltpu.SemaphoreType.DMA((cols,)),
            pltpu.SemaphoreType.DMA((rows,)),
            pltpu.SemaphoreType.DMA((rows,)),
        ],
        compiler_params=pltpu.CompilerParams(collective_id=1, has_side_effects=True),
        cost_estimate=pl.CostEstimate(flops=40_000_000, bytes_accessed=1_000_000, transcendentals=0),
        name="add_diagonals",
    )(sums)


def three_terms(value):
    first = value.astype(BF16)
    rest = value - first.astype(F32)
    second = rest.astype(BF16)
    third = (rest - second.astype(F32)).astype(BF16)
    return jnp.concatenate([first.astype(F32), second.astype(F32), third.astype(F32)], axis=0)


def row_masked(stacked, which):
    line = lax.broadcasted_iota(jnp.int32, stacked.shape, 0) & 7
    return jnp.where(line == which, stacked, 0.0).astype(BF16)


def conjugate_kernel(
    rows, cols, tile_ref, blocks_ref, right_ref, update_ref, residual_ref,
    direction, remainder, answer, row_firsts, col_first, row_second, col_seconds,
    send_row, recv_row, send_col, recv_col, send_row2, recv_row2, send_col2, recv_col2,
):
    row, col = lax.axis_index("row"), lax.axis_index("col")
    enter(rows, cols)
    direction[...] = right_ref[...]
    remainder[...] = right_ref[...]
    answer[...] = jnp.zeros_like(answer)

    def inner(first, second):
        total = first[0] * second[0]
        for r in range(1, rows):
            total = total + first[r] * second[r]
        return jnp.sum(jnp.sum(total, axis=0, keepdims=True), axis=1, keepdims=True)

    start = right_ref[...]
    norm_now = inner(start, start)

    def iteration(step, norm_now):
        parity = lax.rem(step, 2)
        row_first, col_second = row_firsts.at[parity], col_seconds.at[parity]
        rows_part = direction[row]
        cols_part = direction[col // 2, :, pl.ds(pl.multiple_of((col % 2) * LANES, LANES), LANES)]
        row_terms, col_terms = three_terms(rows_part), three_terms(cols_part)
        col_lhs = [row_masked(col_terms, y) for y in range(6)]
        row_lhs = [row_masked(row_terms, x) for x in range(6)]
        line_rows = lax.broadcasted_iota(jnp.int32, (8, 256), 0)
        line_cols = lax.broadcasted_iota(jnp.int32, (8, LANES), 0)
        forward = jnp.zeros((8, 256), F32)
        for y in range(6):
            forward = forward + blocks_ref[y] * jnp.broadcast_to(rows_part[y : y + 1], (8, 256))
        for x in range(6):
            total = None
            for y in range(6):
                part = lax.dot_general(
                    col_lhs[y], tile_ref[x * 6 + y], (((1,), (1,)), ((), ())), preferred_element_type=F32
                )
                total = part if total is None else total + part
            forward = forward + jnp.where(line_rows == x, jnp.sum(total, axis=0, keepdims=True), 0.0)
        row_first[col] = forward
        copies = spread_along("col", cols, row_first, send_row.at[parity], recv_row.at[parity])
        backward = jnp.zeros((8, LANES), F32)
        for y in range(6):
            total = None
            for x in range(6):
                part = jnp.dot(row_lhs[x], tile_ref[x * 6 + y], preferred_element_type=F32)
                total = part if total is None else total + part
            backward = backward + jnp.where(line_cols == y, jnp.sum(total, axis=0, keepdims=True), 0.0)
        col_first[row] = backward
        copies_col = spread_along("row", rows, col_first, send_col, recv_col)
        for copy in copies_col:
            copy.wait()
        col_second[col] = slot_sum(col_first)
        second_copies = spread_along("col", cols, col_second, send_col2.at[parity], recv_col2.at[parity])
        for copy in copies:
            copy.wait()
        row_second[row] = slot_sum(row_first)
        for copy in spread_along("row", rows, row_second, send_row2, recv_row2):
            copy.wait()
        for copy in second_copies:
            copy.wait()
        held = direction[...]
        image = CAMERA_DAMPING * held + row_second[...]
        back = jnp.stack(
            [jnp.concatenate([col_second[2 * r], col_second[2 * r + 1]], axis=1) for r in range(rows)], axis=0
        )
        image = image + back
        step_size = norm_now / inner(held, image)
        answer[...] = answer[...] + step_size[None] * held
        left = remainder[...] - step_size[None] * image
        remainder[...] = left
        norm_next = inner(left, left)
        direction[...] = left + (norm_next / norm_now)[None] * held
        return norm_next

    lax.fori_loop(0, ITERS, iteration, norm_now)
    update_ref[...] = answer[row][:6]
    residual_ref[...] = remainder[row][:6]


def conjugate(tile, blocks, right, rows, cols):
    dma = pltpu.SemaphoreType.DMA
    return pl.pallas_call(
        functools.partial(conjugate_kernel, rows, cols),
        in_specs=[pl.BlockSpec(memory_space=pltpu.VMEM)] * 3,
        out_specs=[pl.BlockSpec(memory_space=pltpu.VMEM)] * 2,
        out_shape=[jax.ShapeDtypeStruct((6, 256), F32)] * 2,
        scratch_shapes=[
            pltpu.VMEM((rows, 8, 256), F32),
            pltpu.VMEM((rows, 8, 256), F32),
            pltpu.VMEM((rows, 8, 256), F32),
            pltpu.VMEM((2, cols, 8, 256), F32),
            pltpu.VMEM((rows, 8, LANES), F32),
            pltpu.VMEM((rows, 8, 256), F32),
            pltpu.VMEM((2, cols, 8, LANES), F32),
            dma((2, cols)), dma((2, cols)), dma((rows,)), dma((rows,)),
            dma((rows,)), dma((rows,)), dma((2, cols)), dma((2, cols)),
        ],
        compiler_params=pltpu.CompilerParams(collective_id=2, has_side_effects=True),
        name="conjugate",
    )(tile, blocks, right)


def shards(cam_jac, pt_jac, resid, partner, count, tile_map):
    rows, cols = lax.axis_size("row"), lax.axis_size("col")
    scn = partner.shape[0]
    device = lax.axis_index("row") * cols + lax.axis_index("col")
    tile_own = lax.dynamic_slice_in_dim(tile_map, device * scn, scn)
    panel, sums = assemble(cam_jac, pt_jac, resid, partner, count, tile_map, tile_own)
    shaped = panel.reshape(LINK, rows * cols, 2, LANES)
    received = lax.all_to_all(shaped, ("row", "col"), split_axis=1, concat_axis=1, tiled=True)
    blocks, right = add_diagonals(sums, rows, cols)
    tile = select_rows(tile_map, received.reshape(LINK, 256, LANES), scn)
    update, residual = conjugate(tile, blocks, right, rows, cols)
    return tile.reshape(6, 6, 256, LANES), update, residual


def solution(mesh):
    return jax.shard_map(
        shards,
        mesh=mesh,
        in_specs=(
            P(None, None, None, ("row", "col"), None),
            P(None, None, None, ("row", "col"), None),
            P(None, None, ("row", "col"), None),
            P(("row", "col"), None),
            P(("row", "col")),
            P(),
        ),
        out_specs=(P(None, None, "row", "col"), P(None, "row"), P(None, "row")),
        check_vma=False,
    )
```

```python
import functools

import jax
import jax.numpy as jnp
from jax import lax
from jax.experimental import pallas as pl
from jax.experimental.pallas import tpu as pltpu
from jax.sharding import PartitionSpec as P

ITERS = 3
CAMERA_DAMPING = 1.0
POINT_DAMPING = 1.0

F32 = jnp.float32
BF16 = jnp.bfloat16
MESH = pl.DeviceIdType.MESH
LANES = 128

LINK = 36
PAIRS = [(x, y) for x in range(6) for y in range(x, 6)]
DIAG = len(PAIRS)
VALUES = 64
GRAD_AT = 24
SUM_ROWS = 32


def pair_index(x, y):
    return PAIRS.index((min(x, y), max(x, y)))


def dot3(first, second):
    total = first[0] * second[0]
    for k in range(1, len(first)):
        total = total + first[k] * second[k]
    return total


def point_chunk(cam_ref, pt_ref, res_ref, active, at):
    def cam(side, i):
        return [cam_ref[side, i, x, :, at].astype(F32) for x in range(6)]

    pa = [[pt_ref[0, i, k, :, at].astype(F32) for k in range(3)] for i in range(2)]
    pb = [[pt_ref[1, i, k, :, at].astype(F32) for k in range(3)] for i in range(2)]
    ea = [res_ref[0, i, :, at].astype(F32) for i in range(2)]
    eb = [res_ref[1, i, :, at].astype(F32) for i in range(2)]

    def hess(m, n):
        return pa[0][m] * pa[0][n] + pa[1][m] * pa[1][n] + (pb[0][m] * pb[0][n] + pb[1][m] * pb[1][n])

    v00, v11, v22 = (hess(k, k) + POINT_DAMPING for k in range(3))
    v01, v02, v12 = hess(0, 1), hess(0, 2), hess(1, 2)
    c00 = v11 * v22 - v12 * v12
    c01 = v02 * v12 - v01 * v22
    c02 = v01 * v12 - v02 * v11
    c11 = v00 * v22 - v02 * v02
    c12 = v01 * v02 - v00 * v12
    c22 = v00 * v11 - v01 * v01
    det = v00 * c00 + v01 * c01 + v02 * c02
    scale = 1.0 / det
    i00, i01, i02 = c00 * scale, c01 * scale, c02 * scale
    i11, i12, i22 = c11 * scale, c12 * scale, c22 * scale
    inv = [[i00, i01, i02], [i01, i11, i12], [i02, i12, i22]]
    q = [-(pa[0][k] * ea[0] + pa[1][k] * ea[1] + (pb[0][k] * eb[0] + pb[1][k] * eb[1])) for k in range(3)]
    pav = [[dot3(pa[i], inv[k]) for k in range(3)] for i in range(2)]
    pbv = [[dot3(pb[i], inv[k]) for k in range(3)] for i in range(2)]

    def schur(pv, p):
        n00 = (1.0 - dot3(pv[0], p[0])) * active
        n01 = -dot3(pv[0], p[1]) * active
        n11 = (1.0 - dot3(pv[1], p[1])) * active
        return [[n00, n01], [n01, n11]]

    naa, nbb = schur(pav, pa), schur(pbv, pb)
    mab = [[-dot3(pav[i], pb[j]) * active for j in range(2)] for i in range(2)]
    ga = [-(ea[i] + dot3(pav[i], q)) * active for i in range(2)]
    gb = [-(eb[i] + dot3(pbv[i], q)) * active for i in range(2)]
    ja = [cam(0, 0), cam(0, 1)]
    jb = [cam(1, 0), cam(1, 1)]

    def quad(left, middle, right, pairs):
        half = [[middle[i][0] * right[0][y] + middle[i][1] * right[1][y] for y in range(6)] for i in range(2)]
        return [left[0][x] * half[0][y] + left[1][x] * half[1][y] for x, y in pairs]

    link = quad(ja, mab, jb, [(x, y) for x in range(6) for y in range(6)])
    diag_other = quad(jb, nbb, jb, PAIRS)
    grad_other = [jb[0][x] * gb[0] + jb[1][x] * gb[1] for x in range(6)]
    diag_own = quad(ja, naa, ja, PAIRS)
    grad_own = [ja[0][x] * ga[0] + ja[1][x] * ga[1] for x in range(6)]
    return link + diag_other + grad_other, diag_own + grad_own


def slot_sum(buffer):
    total = buffer[0]
    for k in range(1, buffer.shape[0]):
        total = total + buffer[k]
    return total


def three_terms(value):
    first = value.astype(BF16)
    rest = value - first.astype(F32)
    second = rest.astype(BF16)
    third = (rest - second.astype(F32)).astype(BF16)
    return jnp.concatenate([first.astype(F32), second.astype(F32), third.astype(F32)], axis=0)


def row_masked(stacked, which):
    line = lax.broadcasted_iota(jnp.int32, stacked.shape, 0) & 7
    return jnp.where(line == which, stacked, 0.0).astype(BF16)


def start_along(axis, n, buffer, send, recv):
    me = lax.axis_index(axis)
    copies = []
    for k in range(1, n):
        copy = pltpu.make_async_remote_copy(
            src_ref=buffer.at[me],
            dst_ref=buffer.at[me],
            send_sem=send.at[k],
            recv_sem=recv.at[k],
            device_id={axis: lax.rem(me + k, n)},
            device_id_type=MESH,
        )
        copy.start()
        copies.append(copy)
    return copies


def finish(copies):
    for copy in copies:
        copy.wait()


def exclusive_or(first, second, bits):
    total = 0
    for k in range(bits):
        total = total + (1 << k) * lax.rem(first // (1 << k) + second // (1 << k), 2)
    return total


def whole_kernel(
    rows, cols,
    map_smem, count_smem, cam_hbm, pt_hbm, res_hbm, partner_hbm, map_ref,
    tile, update_ref, residual_ref,
    cam_ref, pt_ref, res_ref, partner_ref, rank,
    high, low, own_acc, lane_index, group_index, lhs, acc, weave,
    panel, received, sums, parts, selection,
    first_right, second_right, blocks,
    direction, remainder, answer, row_firsts, col_first, row_second, col_seconds,
    input_sems, panel_send, panel_recv, parts_send, parts_recv,
    first_send, first_recv, second_send, second_recv,
    send_row, recv_row, send_col, recv_col, send_row2, recv_row2, send_col2, recv_col2,
):
    row, col = lax.axis_index("row"), lax.axis_index("col")
    me = row * cols + col
    devices = rows * cols
    scn, points = partner_ref.shape
    chunks = points // LANES
    lines = map_ref.shape[0]
    groups = 8

    inputs = [
        pltpu.make_async_copy(source, target, input_sems.at[k])
        for k, (source, target) in enumerate(
            ((cam_hbm, cam_ref), (pt_hbm, pt_ref), (res_hbm, res_ref), (partner_hbm, partner_ref))
        )
    ]
    for copy in inputs:
        copy.start()

    barrier = pltpu.get_barrier_semaphore()

    def greet(k, carry):
        other = lax.rem(me + k, devices)
        pl.semaphore_signal(
            barrier, inc=1, device_id=(other // cols, lax.rem(other, cols)), device_id_type=MESH
        )
        return carry

    lax.fori_loop(1, devices, greet, 0)

    for s in range(scn):
        here = map_smem[me * scn + s]
        total = jnp.int32(0)
        for t in range(scn):
            if t != s:
                total = total + (map_smem[me * scn + t] < here).astype(jnp.int32)
        rank[s] = total

    def scalars_column(ref, offset, shape):
        line = lax.broadcasted_iota(jnp.int32, shape, 0)
        column = jnp.zeros(shape, jnp.int32)
        for s in range(shape[0]):
            column = jnp.where(line == s, ref[offset + s], column)
        return column

    counts = scalars_column(count_smem, 0, (scn, LANES))
    own_acc[...] = jnp.zeros_like(own_acc)
    acc[...] = jnp.zeros_like(acc)
    high[pl.ds((VALUES - 1) * scn, scn), :] = jnp.zeros((scn, points), F32)
    low[pl.ds((VALUES - 1) * scn, scn), :] = jnp.zeros((scn, points), F32)
    for copy in inputs:
        copy.wait()

    def chunk(j, carry):
        at = pl.ds(pl.multiple_of(j * LANES, LANES), LANES)
        slot = lax.broadcasted_iota(jnp.int32, (scn, LANES), 1) + j * LANES
        active = (slot < counts).astype(F32)
        values, own = point_chunk(cam_ref, pt_ref, res_ref, active, at)
        for v, value in enumerate(values):
            top = value.astype(BF16).astype(F32)
            high[pl.ds(v * scn, scn), at] = top
            low[pl.ds(v * scn, scn), at] = value - top
        for v, value in enumerate(own):
            own_acc[v] += value
        partner = partner_ref[:, at]
        which = partner & (LANES - 1)
        line = partner >> 7
        position = jnp.zeros((scn, LANES), jnp.int32)
        for h in range(lines):
            table_row = jnp.broadcast_to(map_ref[h : h + 1, :], (scn, LANES))
            position = jnp.where(line == h, jnp.take_along_axis(table_row, which, axis=1), position)
        column = position >> 7
        lane_index[:, at] = ((column >> 3) << 7) | (position & (LANES - 1))
        group_index[:, at] = column & 7
        return carry

    lax.fori_loop(0, chunks, chunk, 0)
    pl.semaphore_wait(barrier, devices - 1)

    def scatter(s, first, count):
        group_row = jnp.broadcast_to(group_index[pl.ds(s, 1), :], (groups, points))
        keep = group_row == lax.broadcasted_iota(jnp.int32, (groups, points), 0)
        lane_row = lane_index[pl.ds(s, 1), :]
        onehot = jnp.where(
            lane_row == lax.broadcasted_iota(jnp.int32, (256, points), 0), 1.0, 0.0
        ).astype(BF16)
        for part, source in enumerate((high, low)):
            for v in range(0, count, 2):
                pieces = [
                    jnp.where(
                        keep,
                        jnp.broadcast_to(source[pl.ds((first + v + k) * scn + s, 1), :], (groups, points)),
                        0.0,
                    )
                    for k in range(2)
                ]
                lhs[pl.ds((part * count + v) * groups, 2 * groups), :] = jnp.concatenate(pieces, axis=0).astype(BF16)
        result = lax.dot_general(
            lhs[: 2 * count * groups], onehot, (((1,), (1,)), ((), ())), preferred_element_type=F32
        )
        return result[: count * groups] + result[count * groups :]

    panel_view = panel.reshape(LINK, rows, 2, 2 * groups, LANES)

    def link_rows(k, carry):
        target = exclusive_or(row, k, 3)
        for slot in range(2):
            s = jnp.int32(0)
            for t in range(scn):
                s = jnp.where(rank[t] == target * 2 + slot, t, s)
            result = scatter(s, 0, LINK)
            for x in range(LINK):
                for b in range(2):
                    weave[pl.ds((x * 2 + b) * 2 * groups + slot, groups, stride=2), :] = result[
                        x * groups : (x + 1) * groups, b * LANES : (b + 1) * LANES
                    ]
        panel_view[:, target] = weave[...].reshape(LINK, 2, 2 * groups, LANES).astype(BF16)
        return carry

    def send_rows(k, carry):
        target = exclusive_or(row, k, 3)

        def send(j, inner):
            column = exclusive_or(col, j, 4)
            there = target * cols + column

            @pl.when(k * cols + j > 0)
            def _():
                pltpu.make_async_remote_copy(
                    src_ref=panel.at[:, there],
                    dst_ref=received.at[:, me],
                    send_sem=panel_send,
                    recv_sem=panel_recv,
                    device_id=(target, column),
                    device_id_type=MESH,
                ).start()

            return inner

        return lax.fori_loop(0, cols, send, carry)

    def link_and_send(k, carry):
        link_rows(k, 0)
        send_rows(k, 0)
        return carry

    lax.fori_loop(0, 2, link_and_send, 0)
    received[:, me] = panel[:, me]

    def other_sums(s, carry):
        result = scatter(s, LINK, VALUES - LINK)
        for b in range(2):
            acc[pl.ds(b * (VALUES - LINK) * groups, (VALUES - LINK) * groups), :] += result[
                :, b * LANES : (b + 1) * LANES
            ]
        return carry

    lax.fori_loop(0, scn, other_sums, 0)
    lanes = lax.broadcasted_iota(jnp.int32, (scn, LANES), 1)
    own_table = jnp.zeros((scn, LANES), F32)
    for v in range(DIAG + 6):
        total = jnp.sum(own_acc[v], axis=1, keepdims=True)
        own_table = jnp.where(lanes == (v if v < DIAG else GRAD_AT + v - DIAG), total, own_table)
    own_table = own_table.T[:SUM_ROWS]
    own_at = scalars_column(map_smem, me * scn, (scn, LANES))
    zeros = jnp.zeros((3, LANES), F32)
    for b in range(2):
        for h in range(groups):
            column = b * groups + h
            spread = (own_at == lanes + column * LANES).astype(F32)
            own_sum = lax.dot_general(
                own_table, spread, (((1,), (0,)), ((), ())),
                precision=lax.Precision.HIGHEST, preferred_element_type=F32,
            )
            other = acc[pl.ds(b * (VALUES - LINK) * groups + h, VALUES - LINK, stride=groups), :]
            sums[column // 2, :, (column % 2) * LANES : (column % 2 + 1) * LANES] = own_sum + jnp.concatenate(
                [other[:DIAG], zeros, other[DIAG : DIAG + 6], zeros[:2]], axis=0
            )
    part_copies = []
    for k in range(1, rows):
        there = lax.rem(row + k, rows)
        copy = pltpu.make_async_remote_copy(
            src_ref=sums.at[there],
            dst_ref=parts.at[row],
            send_sem=parts_send.at[k],
            recv_sem=parts_recv.at[k],
            device_id={"row": there},
            device_id_type=MESH,
        )
        copy.start()
        part_copies.append(copy)
    parts[row] = sums[row]

    lax.fori_loop(2, 4, link_and_send, 0)
    lax.fori_loop(4, rows, link_rows, 0)

    finish(part_copies)
    total = slot_sum(parts)
    first_right[col] = total[GRAD_AT : GRAD_AT + 8]
    copies = start_along("col", cols, first_right, first_send, first_recv)
    lax.fori_loop(4, 6, send_rows, 0)
    line = lax.broadcasted_iota(jnp.int32, (8, 256), 0)
    for y in range(6):
        block = jnp.zeros((8, 256), F32)
        for x in range(6):
            v = pair_index(x, y)
            block = jnp.where(line == x, jnp.broadcast_to(total[v : v + 1], (8, 256)), block)
        blocks[y] = block

    offset = map_ref[...] - row * 256
    inside = (offset >= 0) & (offset < 256)
    lane = lax.broadcasted_iota(jnp.int32, (lines, LANES), 1)
    least = jnp.where(inside, offset, 256)
    for span in (1, 2, 4, 8):
        ahead = pltpu.roll(least, LANES - span, axis=1)
        behind = pltpu.roll(least, span, axis=1)
        least = jnp.minimum(least, jnp.where((lane & span) == 0, ahead, behind))
    later = (offset != least).astype(jnp.int32)
    source = (lax.broadcasted_iota(jnp.int32, (lines, LANES), 0) * 8 + (lane >> 4)) * 2 + later
    place = jnp.where(inside, offset, -1)
    source = jnp.where(inside, source, -1)
    deep = lax.broadcasted_iota(jnp.int32, (256, LANES), 0)
    chosen = jnp.zeros((256, 256), F32)
    for h in range(lines):
        place_hot = jnp.where(place[h : h + 1] == deep, 1.0, 0.0).astype(BF16)
        source_hot = jnp.where(source[h : h + 1] == deep, 1.0, 0.0).astype(BF16)
        chosen = chosen + lax.dot_general(
            place_hot, source_hot, (((1,), (1,)), ((), ())), preferred_element_type=F32
        )
    selection[...] = chosen.astype(BF16)

    finish(copies)
    second_right[row] = slot_sum(first_right)
    copies = start_along("row", rows, second_right, second_send, second_recv)
    lax.fori_loop(6, rows, send_rows, 0)
    finish(copies)
    start = second_right[...]
    direction[...] = start
    remainder[...] = start
    answer[...] = jnp.zeros_like(answer)

    def inner_product(first, second):
        total = first[0] * second[0]
        for r in range(1, rows):
            total = total + first[r] * second[r]
        return jnp.sum(jnp.sum(total, axis=0, keepdims=True), axis=1, keepdims=True)

    norm_start = inner_product(start, start)

    landed = received.at[:, pl.ds(0, devices - 1)]
    pltpu.make_async_copy(landed, landed, panel_recv).wait()
    received_view = received.reshape(LINK, 2 * devices, LANES)

    def select(x, carry):
        pair = jnp.concatenate([received_view[2 * x], received_view[2 * x + 1]], axis=1)
        chosen_rows = jnp.dot(selection[...], pair, preferred_element_type=F32).astype(BF16)
        tile[2 * x] = chosen_rows[:, :LANES]
        tile[2 * x + 1] = chosen_rows[:, LANES:]
        return carry

    lax.fori_loop(0, LINK // 2, select, 0)

    def iteration(step, norm_now):
        parity = lax.rem(step, 2)
        row_first, col_second = row_firsts.at[parity], col_seconds.at[parity]
        rows_part = direction[row]
        cols_part = direction[col // 2, :, pl.ds(pl.multiple_of(lax.rem(col, 2) * LANES, LANES), LANES)]
        row_terms, col_terms = three_terms(rows_part), three_terms(cols_part)
        col_lhs = [row_masked(col_terms, y) for y in range(6)]
        row_lhs = [row_masked(row_terms, x) for x in range(6)]
        line_rows = lax.broadcasted_iota(jnp.int32, (8, 256), 0)
        line_cols = lax.broadcasted_iota(jnp.int32, (8, LANES), 0)
        forward = jnp.zeros((8, 256), F32)
        for y in range(6):
            forward = forward + blocks[y] * jnp.broadcast_to(rows_part[y : y + 1], (8, 256))
        for x in range(6):
            total = None
            for y in range(6):
                part = lax.dot_general(
                    col_lhs[y], tile[x * 6 + y], (((1,), (1,)), ((), ())), preferred_element_type=F32
                )
                total = part if total is None else total + part
            forward = forward + jnp.where(line_rows == x, jnp.sum(total, axis=0, keepdims=True), 0.0)
        row_first[col] = forward
        copies = start_along("col", cols, row_first, send_row.at[parity], recv_row.at[parity])
        backward = jnp.zeros((8, LANES), F32)
        for y in range(6):
            total = None
            for x in range(6):
                part = jnp.dot(row_lhs[x], tile[x * 6 + y], preferred_element_type=F32)
                total = part if total is None else total + part
            backward = backward + jnp.where(line_cols == y, jnp.sum(total, axis=0, keepdims=True), 0.0)
        col_first[row] = backward
        finish(start_along("row", rows, col_first, send_col, recv_col))
        col_second[col] = slot_sum(col_first)
        second_copies = start_along("col", cols, col_second, send_col2.at[parity], recv_col2.at[parity])
        finish(copies)
        row_second[row] = slot_sum(row_first)
        finish(start_along("row", rows, row_second, send_row2, recv_row2))
        finish(second_copies)
        held = direction[...]
        image = CAMERA_DAMPING * held + row_second[...]
        back = jnp.stack(
            [jnp.concatenate([col_second[2 * r], col_second[2 * r + 1]], axis=1) for r in range(rows)], axis=0
        )
        image = image + back
        step_size = norm_now / inner_product(held, image)
        answer[...] = answer[...] + step_size[None] * held
        left = remainder[...] - step_size[None] * image
        remainder[...] = left
        norm_next = inner_product(left, left)
        direction[...] = left + (norm_next / norm_now)[None] * held
        return norm_next

    lax.fori_loop(0, ITERS, iteration, norm_start)
    update_ref[...] = answer[row][:6]
    residual_ref[...] = remainder[row][:6]
    sent = panel.at[:, pl.ds(0, devices - 1)]
    pltpu.make_async_copy(sent, sent, panel_send).wait()


def store_kernel(*refs):
    count = len(refs) // 2
    sems = refs[-1]
    copies = [pltpu.make_async_copy(refs[k], refs[count + k], sems.at[k]) for k in range(count)]
    for copy in copies:
        copy.start()
    for copy in copies:
        copy.wait()


def store(arrays):
    return pl.pallas_call(
        store_kernel,
        in_specs=[pl.BlockSpec(memory_space=pltpu.VMEM)] * len(arrays),
        out_specs=[pl.BlockSpec(memory_space=pltpu.HBM)] * len(arrays),
        out_shape=[jax.ShapeDtypeStruct(array.shape, array.dtype) for array in arrays],
        scratch_shapes=[pltpu.SemaphoreType.DMA((len(arrays),))],
        compiler_params=pltpu.CompilerParams(vmem_limit_bytes=8 * 1024 * 1024),
        name="store",
    )(*arrays)


def shards(cam_jac, pt_jac, resid, partner, count, tile_map):
    rows, cols = lax.axis_size("row"), lax.axis_size("col")
    scn, points = partner.shape
    devices = rows * cols
    groups = 8
    dma = pltpu.SemaphoreType.DMA
    vmem = pltpu.VMEM
    smem_spec = pl.BlockSpec(memory_space=pltpu.SMEM)
    vmem_spec = pl.BlockSpec(memory_space=pltpu.VMEM)
    hbm_spec = pl.BlockSpec(memory_space=pltpu.HBM)
    coupling, update, residual = pl.pallas_call(
        functools.partial(whole_kernel, rows, cols),
        in_specs=[smem_spec, smem_spec, hbm_spec, hbm_spec, hbm_spec, hbm_spec, vmem_spec],
        out_specs=[vmem_spec] * 3,
        out_shape=[
            jax.ShapeDtypeStruct((LINK, 256, LANES), BF16),
            jax.ShapeDtypeStruct((6, 256), F32),
            jax.ShapeDtypeStruct((6, 256), F32),
        ],
        scratch_shapes=[
            vmem(cam_jac.shape, BF16),
            vmem(pt_jac.shape, BF16),
            vmem(resid.shape, BF16),
            vmem(partner.shape, jnp.int32),
            pltpu.SMEM((scn,), jnp.int32),
            vmem((VALUES * scn, points), F32),
            vmem((VALUES * scn, points), F32),
            vmem((DIAG + 6, scn, LANES), F32),
            vmem((scn, points), jnp.int32),
            vmem((scn, points), jnp.int32),
            vmem((2 * LINK * groups, points), BF16),
            vmem((2 * (VALUES - LINK) * groups, LANES), F32),
            vmem((LINK * 2 * 2 * groups, LANES), F32),
            vmem((LINK, devices, 2, LANES), BF16),
            vmem((LINK, devices, 2, LANES), BF16),
            vmem((rows, SUM_ROWS, 256), F32),
            vmem((rows, SUM_ROWS, 256), F32),
            vmem((256, 256), BF16),
            vmem((cols, 8, 256), F32),
            vmem((rows, 8, 256), F32),
            vmem((6, 8, 256), F32),
            vmem((rows, 8, 256), F32),
            vmem((rows, 8, 256), F32),
            vmem((rows, 8, 256), F32),
            vmem((2, cols, 8, 256), F32),
            vmem((rows, 8, LANES), F32),
            vmem((rows, 8, 256), F32),
            vmem((2, cols, 8, LANES), F32),
            dma((4,)), dma, dma, dma((rows,)), dma((rows,)),
            dma((cols,)), dma((cols,)), dma((rows,)), dma((rows,)),
            dma((2, cols)), dma((2, cols)), dma((rows,)), dma((rows,)),
            dma((rows,)), dma((rows,)), dma((2, cols)), dma((2, cols)),
        ],
        compiler_params=pltpu.CompilerParams(
            collective_id=0, has_side_effects=True, vmem_limit_bytes=48 * 1024 * 1024
        ),
        name="bundle",
    )(
        *(
            pltpu.with_memory_space_constraint(array, pltpu.HBM)
            for array in (tile_map, count, cam_jac, pt_jac, resid, partner, tile_map.reshape(-1, LANES))
        )
    )
    coupling, update, residual = store([coupling, update, residual])
    return coupling.reshape(6, 6, 256, LANES), update, residual


def solution(mesh):
    return jax.shard_map(
        shards,
        mesh=mesh,
        in_specs=(
            P(None, None, None, ("row", "col"), None),
            P(None, None, None, ("row", "col"), None),
            P(None, None, ("row", "col"), None),
            P(("row", "col"), None),
            P(("row", "col")),
            P(),
        ),
        out_specs=(P(None, None, "row", "col"), P(None, "row"), P(None, "row")),
        check_vma=False,
    )
```

```python
import functools

import jax
import jax.numpy as jnp
from jax import lax
from jax.experimental import pallas as pl
from jax.experimental.pallas import tpu as pltpu
from jax.sharding import PartitionSpec as P

ITERS = 3
CAMERA_DAMPING = 1.0
POINT_DAMPING = 1.0

F32 = jnp.float32
BF16 = jnp.bfloat16
MESH = pl.DeviceIdType.MESH
LANES = 128

LINK = 36
PAIRS = [(x, y) for x in range(6) for y in range(x, 6)]
DIAG = len(PAIRS)
VALUES = 64
GRAD_AT = 24
SUM_ROWS = 32


def pair_index(x, y):
    return PAIRS.index((min(x, y), max(x, y)))


def dot3(first, second):
    total = first[0] * second[0]
    for k in range(1, len(first)):
        total = total + first[k] * second[k]
    return total


def point_chunk(cam_ref, pt_ref, res_ref, active, at):
    def cam(side, i):
        return [cam_ref[side, i, x, :, at].astype(F32) for x in range(6)]

    pa = [[pt_ref[0, i, k, :, at].astype(F32) for k in range(3)] for i in range(2)]
    pb = [[pt_ref[1, i, k, :, at].astype(F32) for k in range(3)] for i in range(2)]
    ea = [res_ref[0, i, :, at].astype(F32) for i in range(2)]
    eb = [res_ref[1, i, :, at].astype(F32) for i in range(2)]

    def hess(m, n):
        return pa[0][m] * pa[0][n] + pa[1][m] * pa[1][n] + (pb[0][m] * pb[0][n] + pb[1][m] * pb[1][n])

    v00, v11, v22 = (hess(k, k) + POINT_DAMPING for k in range(3))
    v01, v02, v12 = hess(0, 1), hess(0, 2), hess(1, 2)
    c00 = v11 * v22 - v12 * v12
    c01 = v02 * v12 - v01 * v22
    c02 = v01 * v12 - v02 * v11
    c11 = v00 * v22 - v02 * v02
    c12 = v01 * v02 - v00 * v12
    c22 = v00 * v11 - v01 * v01
    det = v00 * c00 + v01 * c01 + v02 * c02
    scale = 1.0 / det
    i00, i01, i02 = c00 * scale, c01 * scale, c02 * scale
    i11, i12, i22 = c11 * scale, c12 * scale, c22 * scale
    inv = [[i00, i01, i02], [i01, i11, i12], [i02, i12, i22]]
    q = [-(pa[0][k] * ea[0] + pa[1][k] * ea[1] + (pb[0][k] * eb[0] + pb[1][k] * eb[1])) for k in range(3)]
    pav = [[dot3(pa[i], inv[k]) for k in range(3)] for i in range(2)]
    pbv = [[dot3(pb[i], inv[k]) for k in range(3)] for i in range(2)]

    def schur(pv, p):
        n00 = (1.0 - dot3(pv[0], p[0])) * active
        n01 = -dot3(pv[0], p[1]) * active
        n11 = (1.0 - dot3(pv[1], p[1])) * active
        return [[n00, n01], [n01, n11]]

    naa, nbb = schur(pav, pa), schur(pbv, pb)
    mab = [[-dot3(pav[i], pb[j]) * active for j in range(2)] for i in range(2)]
    ga = [-(ea[i] + dot3(pav[i], q)) * active for i in range(2)]
    gb = [-(eb[i] + dot3(pbv[i], q)) * active for i in range(2)]
    ja = [cam(0, 0), cam(0, 1)]
    jb = [cam(1, 0), cam(1, 1)]

    def quad(left, middle, right, pairs):
        half = [[middle[i][0] * right[0][y] + middle[i][1] * right[1][y] for y in range(6)] for i in range(2)]
        return [left[0][x] * half[0][y] + left[1][x] * half[1][y] for x, y in pairs]

    link = quad(ja, mab, jb, [(x, y) for x in range(6) for y in range(6)])
    diag_other = quad(jb, nbb, jb, PAIRS)
    grad_other = [jb[0][x] * gb[0] + jb[1][x] * gb[1] for x in range(6)]
    diag_own = quad(ja, naa, ja, PAIRS)
    grad_own = [ja[0][x] * ga[0] + ja[1][x] * ga[1] for x in range(6)]
    return link + diag_other + grad_other, diag_own + grad_own


def slot_sum(buffer):
    total = buffer[0]
    for k in range(1, buffer.shape[0]):
        total = total + buffer[k]
    return total


def three_terms(value):
    first = value.astype(BF16)
    rest = value - first.astype(F32)
    second = rest.astype(BF16)
    third = (rest - second.astype(F32)).astype(BF16)
    return jnp.concatenate([first.astype(F32), second.astype(F32), third.astype(F32)], axis=0)


def row_masked(stacked, which):
    line = lax.broadcasted_iota(jnp.int32, stacked.shape, 0) & 7
    return jnp.where(line == which, stacked, 0.0).astype(BF16)


def start_along(axis, n, buffer, send, recv):
    me = lax.axis_index(axis)
    copies = []
    for k in range(1, n):
        copy = pltpu.make_async_remote_copy(
            src_ref=buffer.at[me],
            dst_ref=buffer.at[me],
            send_sem=send.at[k],
            recv_sem=recv.at[k],
            device_id={axis: lax.rem(me + k, n)},
            device_id_type=MESH,
        )
        copy.start()
        copies.append(copy)
    return copies


def finish(copies):
    for copy in copies:
        copy.wait()


def exclusive_or(first, second, bits):
    total = 0
    for k in range(bits):
        total = total + (1 << k) * lax.rem(first // (1 << k) + second // (1 << k), 2)
    return total


def whole_kernel(
    rows, cols,
    map_smem, count_smem, cam_hbm, pt_hbm, res_hbm, partner_hbm, map_ref,
    tile, update_ref, residual_ref,
    cam_ref, pt_ref, res_ref, partner_ref, rank,
    high, low, own_acc, lane_index, group_index, lhs, acc, weave,
    panel, received, sums, parts, selection,
    first_right, second_right, blocks,
    direction, remainder, answer, row_firsts, col_first, row_second, col_seconds,
    input_sems, panel_send, panel_recv, parts_send, parts_recv,
    first_send, first_recv, second_send, second_recv,
    send_row, recv_row, send_col, recv_col, send_row2, recv_row2, send_col2, recv_col2,
):
    row, col = lax.axis_index("row"), lax.axis_index("col")
    me = row * cols + col
    devices = rows * cols
    scn, points = partner_ref.shape
    chunks = points // LANES
    lines = map_ref.shape[0]
    groups = 8

    inputs = [
        pltpu.make_async_copy(source, target, input_sems.at[k])
        for k, (source, target) in enumerate(
            ((cam_hbm, cam_ref), (pt_hbm, pt_ref), (res_hbm, res_ref), (partner_hbm, partner_ref))
        )
    ]
    for copy in inputs:
        copy.start()

    barrier = pltpu.get_barrier_semaphore()

    def greet(k, carry):
        other = lax.rem(me + k, devices)
        pl.semaphore_signal(
            barrier, inc=1, device_id=(other // cols, lax.rem(other, cols)), device_id_type=MESH
        )
        return carry

    lax.fori_loop(1, devices, greet, 0)

    for s in range(scn):
        here = map_smem[me * scn + s]
        total = jnp.int32(0)
        for t in range(scn):
            if t != s:
                total = total + (map_smem[me * scn + t] < here).astype(jnp.int32)
        rank[s] = total

    def scalars_column(ref, offset, shape):
        line = lax.broadcasted_iota(jnp.int32, shape, 0)
        column = jnp.zeros(shape, jnp.int32)
        for s in range(shape[0]):
            column = jnp.where(line == s, ref[offset + s], column)
        return column

    counts = scalars_column(count_smem, 0, (scn, LANES))
    own_acc[...] = jnp.zeros_like(own_acc)
    acc[...] = jnp.zeros_like(acc)
    high[pl.ds((VALUES - 1) * scn, scn), :] = jnp.zeros((scn, points), F32)
    low[pl.ds((VALUES - 1) * scn, scn), :] = jnp.zeros((scn, points), F32)
    for copy in inputs:
        copy.wait()

    def chunk(j, carry):
        at = pl.ds(pl.multiple_of(j * LANES, LANES), LANES)
        slot = lax.broadcasted_iota(jnp.int32, (scn, LANES), 1) + j * LANES
        active = (slot < counts).astype(F32)
        values, own = point_chunk(cam_ref, pt_ref, res_ref, active, at)
        for v, value in enumerate(values):
            top = value.astype(BF16).astype(F32)
            high[pl.ds(v * scn, scn), at] = top
            low[pl.ds(v * scn, scn), at] = value - top
        for v, value in enumerate(own):
            own_acc[v] += value
        partner = partner_ref[:, at]
        which = partner & (LANES - 1)
        line = partner >> 7
        position = jnp.zeros((scn, LANES), jnp.int32)
        for h in range(lines):
            table_row = jnp.broadcast_to(map_ref[h : h + 1, :], (scn, LANES))
            position = jnp.where(line == h, jnp.take_along_axis(table_row, which, axis=1), position)
        column = position >> 7
        lane_index[:, at] = ((column >> 3) << 7) | (position & (LANES - 1))
        group_index[:, at] = column & 7
        return carry

    lax.fori_loop(0, chunks, chunk, 0)
    pl.semaphore_wait(barrier, devices - 1)

    def scatter(s, first, count, buffer):
        group_row = jnp.broadcast_to(group_index[pl.ds(s, 1), :], (groups, points))
        keep = group_row == lax.broadcasted_iota(jnp.int32, (groups, points), 0)
        lane_row = lane_index[pl.ds(s, 1), :]
        onehot = jnp.where(
            lane_row == lax.broadcasted_iota(jnp.int32, (256, points), 0), 1.0, 0.0
        ).astype(BF16)
        for part, source in enumerate((high, low)):
            for v in range(0, count, 2):
                pieces = [
                    jnp.where(
                        keep,
                        jnp.broadcast_to(source[pl.ds((first + v + k) * scn + s, 1), :], (groups, points)),
                        0.0,
                    )
                    for k in range(2)
                ]
                lhs[buffer, pl.ds((part * count + v) * groups, 2 * groups), :] = jnp.concatenate(pieces, axis=0).astype(BF16)
        result = lax.dot_general(
            lhs[buffer, : 2 * count * groups], onehot, (((1,), (1,)), ((), ())), preferred_element_type=F32
        )
        return result[: count * groups] + result[count * groups :]

    first_target = exclusive_or(row, lax.rem(col, rows), 3)

    panel_view = panel.reshape(LINK, rows, 2, 2 * groups, LANES)

    def link_rows(k, carry):
        target = exclusive_or(first_target, k, 3)
        for slot in range(2):
            s = jnp.int32(0)
            for t in range(scn):
                s = jnp.where(rank[t] == target * 2 + slot, t, s)
            result = scatter(s, 0, LINK, slot)
            for x in range(LINK):
                for b in range(2):
                    weave[pl.ds((x * 2 + b) * 2 * groups + slot, groups, stride=2), :] = result[
                        x * groups : (x + 1) * groups, b * LANES : (b + 1) * LANES
                    ]
        panel_view[:, target] = weave[...].reshape(LINK, 2, 2 * groups, LANES).astype(BF16)
        return carry

    col_flips = [(1 << k) * (1 - 2 * lax.rem(col // (1 << k), 2)) for k in range(4)]

    def send_rows(k, carry):
        target = exclusive_or(first_target, k, 3)
        for j in range(cols):
            column = col
            for bit in range(4):
                if j >> bit & 1:
                    column = column + col_flips[bit]
            there = target * cols + column

            def send():
                pltpu.make_async_remote_copy(
                    src_ref=panel.at[:, there],
                    dst_ref=received.at[:, me],
                    send_sem=panel_send,
                    recv_sem=panel_recv,
                    device_id=(target, column),
                    device_id_type=MESH,
                ).start()

            if j == 0:
                pl.when(target != row)(send)
            else:
                send()
        return carry

    def link_and_send(k, carry):
        link_rows(k, 0)
        send_rows(k, 0)
        return carry

    lax.fori_loop(0, rows, link_and_send, 0)

    def other_sums(pair, carry):
        result = sum(scatter(pair * 2 + k, LINK, VALUES - LINK, k) for k in range(2))
        for b in range(2):
            acc[pl.ds(b * (VALUES - LINK) * groups, (VALUES - LINK) * groups), :] += result[
                :, b * LANES : (b + 1) * LANES
            ]
        return carry

    lax.fori_loop(0, scn // 2, other_sums, 0)
    lanes = lax.broadcasted_iota(jnp.int32, (scn, LANES), 1)
    own_table = jnp.zeros((scn, LANES), F32)
    for v in range(DIAG + 6):
        total = jnp.sum(own_acc[v], axis=1, keepdims=True)
        own_table = jnp.where(lanes == (v if v < DIAG else GRAD_AT + v - DIAG), total, own_table)
    own_table = own_table.T[:SUM_ROWS]
    own_at = scalars_column(map_smem, me * scn, (scn, LANES))
    zeros = jnp.zeros((3, LANES), F32)
    for b in range(2):
        for h in range(groups):
            column = b * groups + h
            spread = (own_at == lanes + column * LANES).astype(F32)
            own_sum = lax.dot_general(
                own_table, spread, (((1,), (0,)), ((), ())),
                precision=lax.Precision.HIGHEST, preferred_element_type=F32,
            )
            other = acc[pl.ds(b * (VALUES - LINK) * groups + h, VALUES - LINK, stride=groups), :]
            sums[column // 2, :, (column % 2) * LANES : (column % 2 + 1) * LANES] = own_sum + jnp.concatenate(
                [other[:DIAG], zeros, other[DIAG : DIAG + 6], zeros[:2]], axis=0
            )
    part_copies = []
    for k in range(1, rows):
        there = lax.rem(row + k, rows)
        copy = pltpu.make_async_remote_copy(
            src_ref=sums.at[there],
            dst_ref=parts.at[row],
            send_sem=parts_send.at[k],
            recv_sem=parts_recv.at[k],
            device_id={"row": there},
            device_id_type=MESH,
        )
        copy.start()
        part_copies.append(copy)
    parts[row] = sums[row]

    received[:, me] = panel[:, me]

    offset = map_ref[...] - row * 256
    inside = (offset >= 0) & (offset < 256)
    lane = lax.broadcasted_iota(jnp.int32, (lines, LANES), 1)
    least = jnp.where(inside, offset, 256)
    for span in (1, 2, 4, 8):
        ahead = pltpu.roll(least, LANES - span, axis=1)
        behind = pltpu.roll(least, span, axis=1)
        least = jnp.minimum(least, jnp.where((lane & span) == 0, ahead, behind))
    later = (offset != least).astype(jnp.int32)
    source = (lax.broadcasted_iota(jnp.int32, (lines, LANES), 0) * 8 + (lane >> 4)) * 2 + later
    place = jnp.where(inside, offset, -1)
    source = jnp.where(inside, source, -1)
    deep = lax.broadcasted_iota(jnp.int32, (256, LANES), 0)
    chosen = jnp.zeros((256, 256), F32)
    for h in range(lines):
        place_hot = jnp.where(place[h : h + 1] == deep, 1.0, 0.0).astype(BF16)
        source_hot = jnp.where(source[h : h + 1] == deep, 1.0, 0.0).astype(BF16)
        chosen = chosen + lax.dot_general(
            place_hot, source_hot, (((1,), (1,)), ((), ())), preferred_element_type=F32
        )
    selection[...] = chosen.astype(BF16)

    finish(part_copies)
    total = slot_sum(parts)
    first_right[col] = total[GRAD_AT : GRAD_AT + 8]
    copies = start_along("col", cols, first_right, first_send, first_recv)
    line = lax.broadcasted_iota(jnp.int32, (8, 256), 0)
    for y in range(6):
        block = jnp.zeros((8, 256), F32)
        for x in range(6):
            v = pair_index(x, y)
            block = jnp.where(line == x, jnp.broadcast_to(total[v : v + 1], (8, 256)), block)
        blocks[y] = block


    landed = received.at[:, pl.ds(0, devices - 1)]
    pltpu.make_async_copy(landed, landed, panel_recv).wait()
    received_view = received.reshape(LINK, 2 * devices, LANES)

    def select(block, carry):
        for k in range(6):
            x = (block * 6 + k) * 2
            pair = jnp.concatenate([received_view[x], received_view[x + 1]], axis=1)
            chosen_rows = jnp.dot(selection[...], pair, preferred_element_type=F32).astype(BF16)
            tile[x] = chosen_rows[:, :LANES]
            tile[x + 1] = chosen_rows[:, LANES:]
        return carry

    lax.fori_loop(0, LINK // 12, select, 0)

    finish(copies)
    second_right[row] = slot_sum(first_right)
    finish(start_along("row", rows, second_right, second_send, second_recv))
    start = second_right[...]
    direction[...] = start
    remainder[...] = start
    answer[...] = jnp.zeros_like(answer)

    def inner_product(first, second):
        total = first[0] * second[0]
        for r in range(1, rows):
            total = total + first[r] * second[r]
        return jnp.sum(jnp.sum(total, axis=0, keepdims=True), axis=1, keepdims=True)

    norm_start = inner_product(start, start)

    def iteration(step, norm_now):
        parity = lax.rem(step, 2)
        row_first, col_second = row_firsts.at[parity], col_seconds.at[parity]
        rows_part = direction[row]
        cols_part = direction[col // 2, :, pl.ds(pl.multiple_of(lax.rem(col, 2) * LANES, LANES), LANES)]
        row_terms, col_terms = three_terms(rows_part), three_terms(cols_part)
        col_lhs = [row_masked(col_terms, y) for y in range(6)]
        row_lhs = [row_masked(row_terms, x) for x in range(6)]
        line_rows = lax.broadcasted_iota(jnp.int32, (8, 256), 0)
        line_cols = lax.broadcasted_iota(jnp.int32, (8, LANES), 0)
        forward = jnp.zeros((8, 256), F32)
        for y in range(6):
            forward = forward + blocks[y] * jnp.broadcast_to(rows_part[y : y + 1], (8, 256))
        for x in range(6):
            total = None
            for y in range(6):
                part = lax.dot_general(
                    col_lhs[y], tile[x * 6 + y], (((1,), (1,)), ((), ())), preferred_element_type=F32
                )
                total = part if total is None else total + part
            forward = forward + jnp.where(line_rows == x, jnp.sum(total, axis=0, keepdims=True), 0.0)
        row_first[col] = forward
        copies = start_along("col", cols, row_first, send_row.at[parity], recv_row.at[parity])
        backward = jnp.zeros((8, LANES), F32)
        for y in range(6):
            total = None
            for x in range(6):
                part = jnp.dot(row_lhs[x], tile[x * 6 + y], preferred_element_type=F32)
                total = part if total is None else total + part
            backward = backward + jnp.where(line_cols == y, jnp.sum(total, axis=0, keepdims=True), 0.0)
        col_first[row] = backward
        finish(start_along("row", rows, col_first, send_col, recv_col))
        col_second[col] = slot_sum(col_first)
        second_copies = start_along("col", cols, col_second, send_col2.at[parity], recv_col2.at[parity])
        finish(copies)
        row_second[row] = slot_sum(row_first)
        finish(start_along("row", rows, row_second, send_row2, recv_row2))
        finish(second_copies)
        held = direction[...]
        image = CAMERA_DAMPING * held + row_second[...]
        back = jnp.stack(
            [jnp.concatenate([col_second[2 * r], col_second[2 * r + 1]], axis=1) for r in range(rows)], axis=0
        )
        image = image + back
        step_size = norm_now / inner_product(held, image)
        answer[...] = answer[...] + step_size[None] * held
        left = remainder[...] - step_size[None] * image
        remainder[...] = left
        norm_next = inner_product(left, left)
        direction[...] = left + (norm_next / norm_now)[None] * held
        return norm_next

    lax.fori_loop(0, ITERS, iteration, norm_start)
    update_ref[...] = answer[row][:6]
    residual_ref[...] = remainder[row][:6]
    sent = panel.at[:, pl.ds(0, devices - 1)]
    pltpu.make_async_copy(sent, sent, panel_send).wait()


def store_kernel(*refs):
    count = len(refs) // 2
    sems = refs[-1]
    copies = [pltpu.make_async_copy(refs[k], refs[count + k], sems.at[k]) for k in range(count)]
    for copy in copies:
        copy.start()
    for copy in copies:
        copy.wait()


def store(arrays):
    return pl.pallas_call(
        store_kernel,
        in_specs=[pl.BlockSpec(memory_space=pltpu.VMEM)] * len(arrays),
        out_specs=[pl.BlockSpec(memory_space=pltpu.HBM)] * len(arrays),
        out_shape=[jax.ShapeDtypeStruct(array.shape, array.dtype) for array in arrays],
        scratch_shapes=[pltpu.SemaphoreType.DMA((len(arrays),))],
        compiler_params=pltpu.CompilerParams(vmem_limit_bytes=8 * 1024 * 1024),
        name="store",
    )(*arrays)


def shards(cam_jac, pt_jac, resid, partner, count, tile_map):
    rows, cols = lax.axis_size("row"), lax.axis_size("col")
    scn, points = partner.shape
    devices = rows * cols
    groups = 8
    dma = pltpu.SemaphoreType.DMA
    vmem = pltpu.VMEM
    smem_spec = pl.BlockSpec(memory_space=pltpu.SMEM)
    vmem_spec = pl.BlockSpec(memory_space=pltpu.VMEM)
    hbm_spec = pl.BlockSpec(memory_space=pltpu.HBM)
    coupling, update, residual = pl.pallas_call(
        functools.partial(whole_kernel, rows, cols),
        in_specs=[smem_spec, smem_spec, hbm_spec, hbm_spec, hbm_spec, hbm_spec, vmem_spec],
        out_specs=[vmem_spec] * 3,
        out_shape=[
            jax.ShapeDtypeStruct((LINK, 256, LANES), BF16),
            jax.ShapeDtypeStruct((6, 256), F32),
            jax.ShapeDtypeStruct((6, 256), F32),
        ],
        scratch_shapes=[
            vmem(cam_jac.shape, BF16),
            vmem(pt_jac.shape, BF16),
            vmem(resid.shape, BF16),
            vmem(partner.shape, jnp.int32),
            pltpu.SMEM((scn,), jnp.int32),
            vmem((VALUES * scn, points), F32),
            vmem((VALUES * scn, points), F32),
            vmem((DIAG + 6, scn, LANES), F32),
            vmem((scn, points), jnp.int32),
            vmem((scn, points), jnp.int32),
            vmem((2, 2 * LINK * groups, points), BF16),
            vmem((2 * (VALUES - LINK) * groups, LANES), F32),
            vmem((LINK * 2 * 2 * groups, LANES), F32),
            vmem((LINK, devices, 2, LANES), BF16),
            vmem((LINK, devices, 2, LANES), BF16),
            vmem((rows, SUM_ROWS, 256), F32),
            vmem((rows, SUM_ROWS, 256), F32),
            vmem((256, 256), BF16),
            vmem((cols, 8, 256), F32),
            vmem((rows, 8, 256), F32),
            vmem((6, 8, 256), F32),
            vmem((rows, 8, 256), F32),
            vmem((rows, 8, 256), F32),
            vmem((rows, 8, 256), F32),
            vmem((2, cols, 8, 256), F32),
            vmem((rows, 8, LANES), F32),
            vmem((rows, 8, 256), F32),
            vmem((2, cols, 8, LANES), F32),
            dma((4,)), dma, dma, dma((rows,)), dma((rows,)),
            dma((cols,)), dma((cols,)), dma((rows,)), dma((rows,)),
            dma((2, cols)), dma((2, cols)), dma((rows,)), dma((rows,)),
            dma((rows,)), dma((rows,)), dma((2, cols)), dma((2, cols)),
        ],
        compiler_params=pltpu.CompilerParams(
            collective_id=0, has_side_effects=True, vmem_limit_bytes=48 * 1024 * 1024
        ),
        name="bundle",
    )(
        *(
            pltpu.with_memory_space_constraint(array, pltpu.HBM)
            for array in (tile_map, count, cam_jac, pt_jac, resid, partner, tile_map.reshape(-1, LANES))
        )
    )
    coupling, update, residual = store([coupling, update, residual])
    return coupling.reshape(6, 6, 256, LANES), update, residual


def solution(mesh):
    return jax.shard_map(
        shards,
        mesh=mesh,
        in_specs=(
            P(None, None, None, ("row", "col"), None),
            P(None, None, None, ("row", "col"), None),
            P(None, None, ("row", "col"), None),
            P(("row", "col"), None),
            P(("row", "col")),
            P(),
        ),
        out_specs=(P(None, None, "row", "col"), P(None, "row"), P(None, "row")),
        check_vma=False,
    )
```

```python
import functools

import jax
import jax.numpy as jnp
from jax import lax
from jax.experimental import pallas as pl
from jax.experimental.pallas import tpu as pltpu
from jax.sharding import PartitionSpec as P

ITERS = 3
CAMERA_DAMPING = 1.0
POINT_DAMPING = 1.0

F32 = jnp.float32
BF16 = jnp.bfloat16
MESH = pl.DeviceIdType.MESH
LANES = 128

LINK = 36
PAIRS = [(x, y) for x in range(6) for y in range(x, 6)]
DIAG = len(PAIRS)
VALUES = 64
GRAD_AT = 24
SUM_ROWS = 32


def pair_index(x, y):
    return PAIRS.index((min(x, y), max(x, y)))


def dot3(first, second):
    total = first[0] * second[0]
    for k in range(1, len(first)):
        total = total + first[k] * second[k]
    return total


def point_chunk(cam_ref, pt_ref, res_ref, active, at):
    def cam(side, i):
        return [cam_ref[side, i, x, :, at].astype(F32) for x in range(6)]

    pa = [[pt_ref[0, i, k, :, at].astype(F32) for k in range(3)] for i in range(2)]
    pb = [[pt_ref[1, i, k, :, at].astype(F32) for k in range(3)] for i in range(2)]
    ea = [res_ref[0, i, :, at].astype(F32) for i in range(2)]
    eb = [res_ref[1, i, :, at].astype(F32) for i in range(2)]

    def hess(m, n):
        return pa[0][m] * pa[0][n] + pa[1][m] * pa[1][n] + (pb[0][m] * pb[0][n] + pb[1][m] * pb[1][n])

    v00, v11, v22 = (hess(k, k) + POINT_DAMPING for k in range(3))
    v01, v02, v12 = hess(0, 1), hess(0, 2), hess(1, 2)
    c00 = v11 * v22 - v12 * v12
    c01 = v02 * v12 - v01 * v22
    c02 = v01 * v12 - v02 * v11
    c11 = v00 * v22 - v02 * v02
    c12 = v01 * v02 - v00 * v12
    c22 = v00 * v11 - v01 * v01
    det = v00 * c00 + v01 * c01 + v02 * c02
    scale = 1.0 / det
    i00, i01, i02 = c00 * scale, c01 * scale, c02 * scale
    i11, i12, i22 = c11 * scale, c12 * scale, c22 * scale
    inv = [[i00, i01, i02], [i01, i11, i12], [i02, i12, i22]]
    q = [-(pa[0][k] * ea[0] + pa[1][k] * ea[1] + (pb[0][k] * eb[0] + pb[1][k] * eb[1])) for k in range(3)]
    pav = [[dot3(pa[i], inv[k]) for k in range(3)] for i in range(2)]
    pbv = [[dot3(pb[i], inv[k]) for k in range(3)] for i in range(2)]

    def schur(pv, p):
        n00 = (1.0 - dot3(pv[0], p[0])) * active
        n01 = -dot3(pv[0], p[1]) * active
        n11 = (1.0 - dot3(pv[1], p[1])) * active
        return [[n00, n01], [n01, n11]]

    naa, nbb = schur(pav, pa), schur(pbv, pb)
    mab = [[-dot3(pav[i], pb[j]) * active for j in range(2)] for i in range(2)]
    ga = [-(ea[i] + dot3(pav[i], q)) * active for i in range(2)]
    gb = [-(eb[i] + dot3(pbv[i], q)) * active for i in range(2)]
    ja = [cam(0, 0), cam(0, 1)]
    jb = [cam(1, 0), cam(1, 1)]

    def quad(left, middle, right, pairs):
        half = [[middle[i][0] * right[0][y] + middle[i][1] * right[1][y] for y in range(6)] for i in range(2)]
        return [left[0][x] * half[0][y] + left[1][x] * half[1][y] for x, y in pairs]

    link = quad(ja, mab, jb, [(x, y) for x in range(6) for y in range(6)])
    diag_other = quad(jb, nbb, jb, PAIRS)
    grad_other = [jb[0][x] * gb[0] + jb[1][x] * gb[1] for x in range(6)]
    diag_own = quad(ja, naa, ja, PAIRS)
    grad_own = [ja[0][x] * ga[0] + ja[1][x] * ga[1] for x in range(6)]
    return link + diag_other + grad_other, diag_own + grad_own


def slot_sum(buffer):
    total = buffer[0]
    for k in range(1, buffer.shape[0]):
        total = total + buffer[k]
    return total


def three_terms(value):
    first = value.astype(BF16)
    rest = value - first.astype(F32)
    second = rest.astype(BF16)
    third = (rest - second.astype(F32)).astype(BF16)
    return jnp.concatenate([first.astype(F32), second.astype(F32), third.astype(F32)], axis=0)


def row_masked(stacked, which):
    line = lax.broadcasted_iota(jnp.int32, stacked.shape, 0) & 7
    return jnp.where(line == which, stacked, 0.0).astype(BF16)


def xor_flips(index, bits):
    return [(1 << k) * (1 - 2 * lax.rem(index // (1 << k), 2)) for k in range(bits)]


def flipped(index, flips, which):
    for k, flip in enumerate(flips):
        if which >> k & 1:
            index = index + flip
    return index


COL_ORDER = (11, 10, 9, 8, 7, 6, 15, 14, 3, 2, 5, 4, 13, 12, 1)
ROW_ORDER = (5, 4, 3, 7, 1, 2, 6)


def start_along(axis, me, flips, order, buffer, send, recv):
    for which in order:
        pltpu.make_async_remote_copy(
            src_ref=buffer.at[me],
            dst_ref=buffer.at[me],
            send_sem=send,
            recv_sem=recv,
            device_id={axis: flipped(me, flips, which)},
            device_id_type=MESH,
        ).start()


def wait_slots(buffer, sem):
    slots = buffer.at[pl.ds(0, buffer.shape[0] - 1)]
    pltpu.make_async_copy(slots, slots, sem).wait()


def exclusive_or(first, second, bits):
    total = 0
    for k in range(bits):
        total = total + (1 << k) * lax.rem(first // (1 << k) + second // (1 << k), 2)
    return total


def whole_kernel(
    rows, cols,
    map_hbm, count_hbm, cam_hbm, pt_hbm, res_hbm, partner_hbm, table_hbm,
    tile, update_ref, residual_ref,
    map_smem, count_smem, map_ref, cam_ref, pt_ref, res_ref, partner_ref, rank,
    high, low, own_acc, lane_index, group_index, lhs, acc, weave,
    panel, received, sums, grads, grad_parts, parts, selection,
    first_right, second_right, blocks,
    direction, remainder, answer, row_firsts, col_first, row_second, col_seconds,
    input_sems, panel_send, panel_recv, parts_send, parts_recv,
    first_send, first_recv, second_send, second_recv,
    send_row, recv_row, send_col, recv_col, send_row2, recv_row2, send_col2, recv_col2,
):
    row, col = lax.axis_index("row"), lax.axis_index("col")
    me = row * cols + col
    devices = rows * cols
    row_flips, col_flips = xor_flips(row, 3), xor_flips(col, 4)
    spread_row = functools.partial(start_along, "col", col, col_flips, COL_ORDER)
    spread_col = functools.partial(start_along, "row", row, row_flips, ROW_ORDER)
    scn, points = partner_ref.shape
    chunks = points // LANES
    lines = map_ref.shape[0]
    groups = 8

    inputs = [
        pltpu.make_async_copy(source, target, input_sems.at[k])
        for k, (source, target) in enumerate(
            (
                (map_hbm, map_smem), (count_hbm, count_smem), (table_hbm, map_ref),
                (pt_hbm, pt_ref), (cam_hbm, cam_ref), (res_hbm, res_ref), (partner_hbm, partner_ref),
            )
        )
    ]
    for copy in inputs:
        copy.start()

    barrier = pltpu.get_barrier_semaphore()

    def greet(k, carry):
        other = lax.rem(me + k, devices)
        pl.semaphore_signal(
            barrier, inc=1, device_id=(other // cols, lax.rem(other, cols)), device_id_type=MESH
        )
        return carry

    lax.fori_loop(1, devices, greet, 0)
    own_acc[...] = jnp.zeros_like(own_acc)
    acc[...] = jnp.zeros_like(acc)
    high[pl.ds((VALUES - 1) * scn, scn), :] = jnp.zeros((scn, points), F32)
    low[pl.ds((VALUES - 1) * scn, scn), :] = jnp.zeros((scn, points), F32)
    for copy in inputs:
        copy.wait()

    for s in range(scn):
        here = map_smem[me * scn + s]
        total = jnp.int32(0)
        for t in range(scn):
            if t != s:
                total = total + (map_smem[me * scn + t] < here).astype(jnp.int32)
        rank[s] = total

    def scalars_column(ref, offset, shape):
        line = lax.broadcasted_iota(jnp.int32, shape, 0)
        column = jnp.zeros(shape, jnp.int32)
        for s in range(shape[0]):
            column = jnp.where(line == s, ref[offset + s], column)
        return column

    counts = scalars_column(count_smem, 0, (scn, LANES))

    def chunk(j, carry):
        at = pl.ds(pl.multiple_of(j * LANES, LANES), LANES)
        slot = lax.broadcasted_iota(jnp.int32, (scn, LANES), 1) + j * LANES
        active = (slot < counts).astype(F32)
        values, own = point_chunk(cam_ref, pt_ref, res_ref, active, at)
        for v, value in enumerate(values):
            top = value.astype(BF16).astype(F32)
            high[pl.ds(v * scn, scn), at] = top
            low[pl.ds(v * scn, scn), at] = value - top
        for v, value in enumerate(own):
            own_acc[v] += value
        partner = partner_ref[:, at]
        which = partner & (LANES - 1)
        line = partner >> 7
        position = jnp.zeros((scn, LANES), jnp.int32)
        for h in range(lines):
            table_row = jnp.broadcast_to(map_ref[h : h + 1, :], (scn, LANES))
            position = jnp.where(line == h, jnp.take_along_axis(table_row, which, axis=1), position)
        column = position >> 7
        lane_index[:, at] = ((column >> 3) << 7) | (position & (LANES - 1))
        group_index[:, at] = column & 7
        return carry

    lax.fori_loop(0, chunks, chunk, 0)

    def scatter(s, first, count, buffer):
        group_row = jnp.broadcast_to(group_index[pl.ds(s, 1), :], (groups, points))
        keep = group_row == lax.broadcasted_iota(jnp.int32, (groups, points), 0)
        lane_row = lane_index[pl.ds(s, 1), :]
        onehot = jnp.where(
            lane_row == lax.broadcasted_iota(jnp.int32, (256, points), 0), 1.0, 0.0
        ).astype(BF16)
        for part, source in enumerate((high, low)):
            for v in range(0, count, 2):
                pieces = [
                    jnp.where(
                        keep,
                        jnp.broadcast_to(source[pl.ds((first + v + k) * scn + s, 1), :], (groups, points)),
                        0.0,
                    )
                    for k in range(2)
                ]
                lhs[buffer, pl.ds((part * count + v) * groups, 2 * groups), :] = jnp.concatenate(pieces, axis=0).astype(BF16)
        result = lax.dot_general(
            lhs[buffer, : 2 * count * groups], onehot, (((1,), (1,)), ((), ())), preferred_element_type=F32
        )
        return result[: count * groups] + result[count * groups :]

    first_target = exclusive_or(row, lax.rem(col, rows), 3)

    panel_view = panel.reshape(LINK, rows, 2, 2 * groups, LANES)

    def link_rows(k, carry):
        target = exclusive_or(first_target, k, 3)
        for slot in range(2):
            s = jnp.int32(0)
            for t in range(scn):
                s = jnp.where(rank[t] == target * 2 + slot, t, s)
            result = scatter(s, 0, LINK, slot)
            for x in range(LINK):
                for b in range(2):
                    weave[pl.ds((x * 2 + b) * 2 * groups + slot, groups, stride=2), :] = result[
                        x * groups : (x + 1) * groups, b * LANES : (b + 1) * LANES
                    ]
        panel_view[:, target] = weave[...].reshape(LINK, 2, 2 * groups, LANES).astype(BF16)
        return carry

    def send_rows(k, carry):
        target = exclusive_or(first_target, k, 3)
        for j in range(cols):
            column = flipped(col, col_flips, j)
            there = target * cols + column

            def send():
                pltpu.make_async_remote_copy(
                    src_ref=panel.at[:, there],
                    dst_ref=received.at[:, me],
                    send_sem=panel_send,
                    recv_sem=panel_recv,
                    device_id=(target, column),
                    device_id_type=MESH,
                ).start()

            if j == 0:
                pl.when(target != row)(send)
            else:
                send()
        return carry

    def link_and_send(k, carry):
        link_rows(k, 0)
        send_rows(k, 0)
        return carry

    link_rows(0, 0)
    pl.semaphore_wait(barrier, devices - 1)
    send_rows(0, 0)

    lanes = lax.broadcasted_iota(jnp.int32, (scn, LANES), 1)
    own_table = jnp.zeros((scn, LANES), F32)
    for v in range(DIAG + 6):
        total = jnp.sum(own_acc[v], axis=1, keepdims=True)
        own_table = jnp.where(lanes == (v if v < DIAG else GRAD_AT + v - DIAG), total, own_table)
    own_table = own_table.T[:SUM_ROWS]
    own_at = scalars_column(map_smem, me * scn, (scn, LANES))
    for column in range(2 * groups):
        spread = (own_at == lanes + column * LANES).astype(F32)
        sums[column // 2, :, (column % 2) * LANES : (column % 2 + 1) * LANES] = lax.dot_general(
            own_table, spread, (((1,), (0,)), ((), ())),
            precision=lax.Precision.HIGHEST, preferred_element_type=F32,
        )

    def other_sums(first, count):
        acc[...] = jnp.zeros_like(acc)

        def pair_sums(pair, carry):
            result = sum(scatter(pair * 2 + k, first, count, k) for k in range(2))
            for b in range(2):
                acc[pl.ds(b * (VALUES - LINK) * groups, count * groups), :] += result[
                    :, b * LANES : (b + 1) * LANES
                ]
            return carry

        lax.fori_loop(0, scn // 2, pair_sums, 0)

    def other_rows(column, count):
        return acc[pl.ds(column // groups * (VALUES - LINK) * groups + column % groups, count, stride=groups), :]

    other_sums(LINK + DIAG, 6)
    zeros = jnp.zeros((3, LANES), F32)
    for column in range(2 * groups):
        lane = slice((column % 2) * LANES, (column % 2 + 1) * LANES)
        grads[column // 2, :, lane] = sums[column // 2, GRAD_AT:, lane] + jnp.concatenate(
            [other_rows(column, 6), zeros[:2]], axis=0
        )

    def start_parts(source, target, send, recv):
        for which in ROW_ORDER:
            there = flipped(row, row_flips, which)
            pltpu.make_async_remote_copy(
                src_ref=source.at[there],
                dst_ref=target.at[row],
                send_sem=send,
                recv_sem=recv,
                device_id={"row": there},
                device_id_type=MESH,
            ).start()

    start_parts(grads, grad_parts, parts_send.at[0], parts_recv.at[0])
    grad_parts[row] = grads[row]
    lax.fori_loop(1, 3, link_and_send, 0)
    wait_slots(grad_parts, parts_recv.at[0])
    first_right[col] = slot_sum(grad_parts)
    spread_row(first_right, first_send, first_recv)
    lax.fori_loop(3, rows, link_and_send, 0)
    received[:, me] = panel[:, me]
    wait_slots(first_right, first_recv)
    second_right[row] = slot_sum(first_right)
    spread_col(second_right, second_send, second_recv)

    other_sums(LINK, DIAG + 1)
    for column in range(2 * groups):
        lane = slice((column % 2) * LANES, (column % 2 + 1) * LANES)
        sums[column // 2, :GRAD_AT, lane] += jnp.concatenate([other_rows(column, DIAG), zeros], axis=0)
    start_parts(sums.at[:, pl.ds(0, GRAD_AT)], parts, parts_send.at[1], parts_recv.at[1])
    parts[row] = sums[row, :GRAD_AT]

    offset = map_ref[...] - row * 256
    inside = (offset >= 0) & (offset < 256)
    lane = lax.broadcasted_iota(jnp.int32, (lines, LANES), 1)
    least = jnp.where(inside, offset, 256)
    for span in (1, 2, 4, 8):
        ahead = pltpu.roll(least, LANES - span, axis=1)
        behind = pltpu.roll(least, span, axis=1)
        least = jnp.minimum(least, jnp.where((lane & span) == 0, ahead, behind))
    later = (offset != least).astype(jnp.int32)
    source = (lax.broadcasted_iota(jnp.int32, (lines, LANES), 0) * 8 + (lane >> 4)) * 2 + later
    place = jnp.where(inside, offset, -1)
    source = jnp.where(inside, source, -1)
    deep = lax.broadcasted_iota(jnp.int32, (256, LANES), 0)
    chosen = jnp.zeros((256, 256), F32)
    for h in range(lines):
        place_hot = jnp.where(place[h : h + 1] == deep, 1.0, 0.0).astype(BF16)
        source_hot = jnp.where(source[h : h + 1] == deep, 1.0, 0.0).astype(BF16)
        chosen = chosen + lax.dot_general(
            place_hot, source_hot, (((1,), (1,)), ((), ())), preferred_element_type=F32
        )
    selection[...] = chosen.astype(BF16)

    wait_slots(second_right, second_recv)
    start = second_right[...]
    direction[...] = start
    remainder[...] = start
    answer[...] = jnp.zeros_like(answer)

    def inner_product(first, second):
        total = first[0] * second[0]
        for r in range(1, rows):
            total = total + first[r] * second[r]
        return jnp.sum(jnp.sum(total, axis=0, keepdims=True), axis=1, keepdims=True)

    norm_start = inner_product(start, start)
    wait_slots(parts, parts_recv.at[1])
    total = slot_sum(parts)
    line = lax.broadcasted_iota(jnp.int32, (8, 256), 0)
    for y in range(6):
        block = jnp.zeros((8, 256), F32)
        for x in range(6):
            v = pair_index(x, y)
            block = jnp.where(line == x, jnp.broadcast_to(total[v : v + 1], (8, 256)), block)
        blocks[y] = block


    landed = received.at[:, pl.ds(0, devices - 1)]
    pltpu.make_async_copy(landed, landed, panel_recv).wait()
    received_view = received.reshape(LINK, 2 * devices, LANES)

    def select(block, carry):
        for k in range(6):
            x = (block * 6 + k) * 2
            pair = jnp.concatenate([received_view[x], received_view[x + 1]], axis=1)
            chosen_rows = jnp.dot(selection[...], pair, preferred_element_type=F32).astype(BF16)
            tile[x] = chosen_rows[:, :LANES]
            tile[x + 1] = chosen_rows[:, LANES:]
        return carry

    lax.fori_loop(0, LINK // 12, select, 0)

    def iteration(step, norm_now):
        parity = lax.rem(step, 2)
        row_first, col_second = row_firsts.at[parity], col_seconds.at[parity]
        rows_part = direction[row]
        cols_part = direction[col // 2, :, pl.ds(pl.multiple_of(lax.rem(col, 2) * LANES, LANES), LANES)]
        row_terms, col_terms = three_terms(rows_part), three_terms(cols_part)
        col_lhs = [row_masked(col_terms, y) for y in range(6)]
        row_lhs = [row_masked(row_terms, x) for x in range(6)]
        line_rows = lax.broadcasted_iota(jnp.int32, (8, 256), 0)
        line_cols = lax.broadcasted_iota(jnp.int32, (8, LANES), 0)
        forward = jnp.zeros((8, 256), F32)
        for y in range(6):
            forward = forward + blocks[y] * jnp.broadcast_to(rows_part[y : y + 1], (8, 256))
        for x in range(6):
            total = None
            for y in range(6):
                part = lax.dot_general(
                    col_lhs[y], tile[x * 6 + y], (((1,), (1,)), ((), ())), preferred_element_type=F32
                )
                total = part if total is None else total + part
            forward = forward + jnp.where(line_rows == x, jnp.sum(total, axis=0, keepdims=True), 0.0)
        row_first[col] = forward
        spread_row(row_first, send_row.at[parity], recv_row.at[parity])
        backward = jnp.zeros((8, LANES), F32)
        for y in range(6):
            total = None
            for x in range(6):
                part = jnp.dot(row_lhs[x], tile[x * 6 + y], preferred_element_type=F32)
                total = part if total is None else total + part
            backward = backward + jnp.where(line_cols == y, jnp.sum(total, axis=0, keepdims=True), 0.0)
        col_first[row] = backward
        spread_col(col_first, send_col, recv_col)
        wait_slots(col_first, recv_col)
        col_second[col] = slot_sum(col_first)
        spread_row(col_second, send_col2.at[parity], recv_col2.at[parity])
        wait_slots(row_first, recv_row.at[parity])
        row_second[row] = slot_sum(row_first)
        spread_col(row_second, send_row2, recv_row2)
        wait_slots(row_second, recv_row2)
        wait_slots(col_second, recv_col2.at[parity])
        wait_slots(row_first, send_row.at[parity])
        wait_slots(col_first, send_col)
        wait_slots(row_second, send_row2)
        wait_slots(col_second, send_col2.at[parity])
        held = direction[...]
        image = CAMERA_DAMPING * held + row_second[...]
        back = jnp.stack(
            [jnp.concatenate([col_second[2 * r], col_second[2 * r + 1]], axis=1) for r in range(rows)], axis=0
        )
        image = image + back
        step_size = norm_now / inner_product(held, image)
        answer[...] = answer[...] + step_size[None] * held
        left = remainder[...] - step_size[None] * image
        remainder[...] = left
        norm_next = inner_product(left, left)
        direction[...] = left + (norm_next / norm_now)[None] * held
        return norm_next

    lax.fori_loop(0, ITERS, iteration, norm_start)
    update_ref[...] = answer[row][:6]
    residual_ref[...] = remainder[row][:6]
    sent = panel.at[:, pl.ds(0, devices - 1)]
    pltpu.make_async_copy(sent, sent, panel_send).wait()
    wait_slots(grad_parts, parts_send.at[0])
    wait_slots(parts, parts_send.at[1])
    wait_slots(first_right, first_send)
    wait_slots(second_right, second_send)


def store_kernel(*refs):
    count = len(refs) // 2
    sems = refs[-1]
    copies = [pltpu.make_async_copy(refs[k], refs[count + k], sems.at[k]) for k in range(count)]
    for copy in copies:
        copy.start()
    for copy in copies:
        copy.wait()


def store(arrays):
    return pl.pallas_call(
        store_kernel,
        in_specs=[pl.BlockSpec(memory_space=pltpu.VMEM)] * len(arrays),
        out_specs=[pl.BlockSpec(memory_space=pltpu.HBM)] * len(arrays),
        out_shape=[jax.ShapeDtypeStruct(array.shape, array.dtype) for array in arrays],
        scratch_shapes=[pltpu.SemaphoreType.DMA((len(arrays),))],
        compiler_params=pltpu.CompilerParams(vmem_limit_bytes=8 * 1024 * 1024),
        name="store",
    )(*arrays)


def shards(cam_jac, pt_jac, resid, partner, count, tile_map):
    rows, cols = lax.axis_size("row"), lax.axis_size("col")
    scn, points = partner.shape
    devices = rows * cols
    groups = 8
    dma = pltpu.SemaphoreType.DMA
    vmem = pltpu.VMEM
    vmem_spec = pl.BlockSpec(memory_space=pltpu.VMEM)
    hbm_spec = pl.BlockSpec(memory_space=pltpu.HBM)
    coupling, update, residual = pl.pallas_call(
        functools.partial(whole_kernel, rows, cols),
        in_specs=[hbm_spec] * 7,
        out_specs=[vmem_spec] * 3,
        out_shape=[
            jax.ShapeDtypeStruct((LINK, 256, LANES), BF16),
            jax.ShapeDtypeStruct((6, 256), F32),
            jax.ShapeDtypeStruct((6, 256), F32),
        ],
        scratch_shapes=[
            pltpu.SMEM(tile_map.shape, jnp.int32),
            pltpu.SMEM(count.shape, jnp.int32),
            vmem((tile_map.shape[0] // LANES, LANES), jnp.int32),
            vmem(cam_jac.shape, BF16),
            vmem(pt_jac.shape, BF16),
            vmem(resid.shape, BF16),
            vmem(partner.shape, jnp.int32),
            pltpu.SMEM((scn,), jnp.int32),
            vmem((VALUES * scn, points), F32),
            vmem((VALUES * scn, points), F32),
            vmem((DIAG + 6, scn, LANES), F32),
            vmem((scn, points), jnp.int32),
            vmem((scn, points), jnp.int32),
            vmem((2, 2 * LINK * groups, points), BF16),
            vmem((2 * (VALUES - LINK) * groups, LANES), F32),
            vmem((LINK * 2 * 2 * groups, LANES), F32),
            vmem((LINK, devices, 2, LANES), BF16),
            vmem((LINK, devices, 2, LANES), BF16),
            vmem((rows, SUM_ROWS, 256), F32),
            vmem((rows, 8, 256), F32),
            vmem((rows, 8, 256), F32),
            vmem((rows, GRAD_AT, 256), F32),
            vmem((256, 256), BF16),
            vmem((cols, 8, 256), F32),
            vmem((rows, 8, 256), F32),
            vmem((6, 8, 256), F32),
            vmem((rows, 8, 256), F32),
            vmem((rows, 8, 256), F32),
            vmem((rows, 8, 256), F32),
            vmem((2, cols, 8, 256), F32),
            vmem((rows, 8, LANES), F32),
            vmem((rows, 8, 256), F32),
            vmem((2, cols, 8, LANES), F32),
            dma((7,)), dma, dma, dma((2,)), dma((2,)),
            dma, dma, dma, dma,
            dma((2,)), dma((2,)), dma, dma, dma, dma, dma((2,)), dma((2,)),
        ],
        compiler_params=pltpu.CompilerParams(
            collective_id=0, has_side_effects=True, vmem_limit_bytes=48 * 1024 * 1024
        ),
        name="bundle",
    )(
        *(
            pltpu.with_memory_space_constraint(array, pltpu.HBM)
            for array in (tile_map, count, cam_jac, pt_jac, resid, partner, tile_map.reshape(-1, LANES))
        )
    )
    coupling, update, residual = store([coupling, update, residual])
    return coupling.reshape(6, 6, 256, LANES), update, residual


def solution(mesh):
    return jax.shard_map(
        shards,
        mesh=mesh,
        in_specs=(
            P(None, None, None, ("row", "col"), None),
            P(None, None, None, ("row", "col"), None),
            P(None, None, ("row", "col"), None),
            P(("row", "col"), None),
            P(("row", "col")),
            P(),
        ),
        out_specs=(P(None, None, "row", "col"), P(None, "row"), P(None, "row")),
        check_vma=False,
    )
```

```python
import functools

import jax
import jax.numpy as jnp
from jax import lax
from jax.experimental import pallas as pl
from jax.experimental.pallas import tpu as pltpu
from jax.sharding import PartitionSpec as P

ITERS = 3
CAMERA_DAMPING = 1.0
POINT_DAMPING = 1.0

F32 = jnp.float32
BF16 = jnp.bfloat16
MESH = pl.DeviceIdType.MESH
LANES = 128

LINK = 36
PAIRS = [(x, y) for x in range(6) for y in range(x, 6)]
DIAG = len(PAIRS)
VALUES = 64
GRAD_AT = 24
SUM_ROWS = 32


def pair_index(x, y):
    return PAIRS.index((min(x, y), max(x, y)))


def dot3(first, second):
    total = first[0] * second[0]
    for k in range(1, len(first)):
        total = total + first[k] * second[k]
    return total


def point_chunk(cam_ref, pt_ref, res_ref, active, at):
    def cam(side, i):
        return [cam_ref[side, i, x, :, at].astype(F32) for x in range(6)]

    pa = [[pt_ref[0, i, k, :, at].astype(F32) for k in range(3)] for i in range(2)]
    pb = [[pt_ref[1, i, k, :, at].astype(F32) for k in range(3)] for i in range(2)]
    ea = [res_ref[0, i, :, at].astype(F32) for i in range(2)]
    eb = [res_ref[1, i, :, at].astype(F32) for i in range(2)]

    def hess(m, n):
        return pa[0][m] * pa[0][n] + pa[1][m] * pa[1][n] + (pb[0][m] * pb[0][n] + pb[1][m] * pb[1][n])

    v00, v11, v22 = (hess(k, k) + POINT_DAMPING for k in range(3))
    v01, v02, v12 = hess(0, 1), hess(0, 2), hess(1, 2)
    c00 = v11 * v22 - v12 * v12
    c01 = v02 * v12 - v01 * v22
    c02 = v01 * v12 - v02 * v11
    c11 = v00 * v22 - v02 * v02
    c12 = v01 * v02 - v00 * v12
    c22 = v00 * v11 - v01 * v01
    det = v00 * c00 + v01 * c01 + v02 * c02
    scale = 1.0 / det
    i00, i01, i02 = c00 * scale, c01 * scale, c02 * scale
    i11, i12, i22 = c11 * scale, c12 * scale, c22 * scale
    inv = [[i00, i01, i02], [i01, i11, i12], [i02, i12, i22]]
    q = [-(pa[0][k] * ea[0] + pa[1][k] * ea[1] + (pb[0][k] * eb[0] + pb[1][k] * eb[1])) for k in range(3)]
    pav = [[dot3(pa[i], inv[k]) for k in range(3)] for i in range(2)]
    pbv = [[dot3(pb[i], inv[k]) for k in range(3)] for i in range(2)]

    def schur(pv, p):
        n00 = (1.0 - dot3(pv[0], p[0])) * active
        n01 = -dot3(pv[0], p[1]) * active
        n11 = (1.0 - dot3(pv[1], p[1])) * active
        return [[n00, n01], [n01, n11]]

    naa, nbb = schur(pav, pa), schur(pbv, pb)
    mab = [[-dot3(pav[i], pb[j]) * active for j in range(2)] for i in range(2)]
    ga = [-(ea[i] + dot3(pav[i], q)) * active for i in range(2)]
    gb = [-(eb[i] + dot3(pbv[i], q)) * active for i in range(2)]
    ja = [cam(0, 0), cam(0, 1)]
    jb = [cam(1, 0), cam(1, 1)]

    def quad(left, middle, right, pairs):
        half = [[middle[i][0] * right[0][y] + middle[i][1] * right[1][y] for y in range(6)] for i in range(2)]
        return [left[0][x] * half[0][y] + left[1][x] * half[1][y] for x, y in pairs]

    link = quad(ja, mab, jb, [(x, y) for x in range(6) for y in range(6)])
    diag_other = quad(jb, nbb, jb, PAIRS)
    grad_other = [jb[0][x] * gb[0] + jb[1][x] * gb[1] for x in range(6)]
    diag_own = quad(ja, naa, ja, PAIRS)
    grad_own = [ja[0][x] * ga[0] + ja[1][x] * ga[1] for x in range(6)]
    return link + diag_other + grad_other, diag_own + grad_own


def slot_sum(buffer):
    total = buffer[0]
    for k in range(1, buffer.shape[0]):
        total = total + buffer[k]
    return total


def three_terms(value):
    first = value.astype(BF16)
    rest = value - first.astype(F32)
    second = rest.astype(BF16)
    third = (rest - second.astype(F32)).astype(BF16)
    return jnp.concatenate([first.astype(F32), second.astype(F32), third.astype(F32)], axis=0)


def row_masked(stacked, which):
    line = lax.broadcasted_iota(jnp.int32, stacked.shape, 0) & 7
    return jnp.where(line == which, stacked, 0.0).astype(BF16)


def xor_flips(index, bits):
    return [(1 << k) * (1 - 2 * lax.rem(index // (1 << k), 2)) for k in range(bits)]


def flipped(index, flips, which):
    for k, flip in enumerate(flips):
        if which >> k & 1:
            index = index + flip
    return index


COL_ORDER = (11, 10, 9, 8, 7, 6, 15, 14, 3, 2, 5, 4, 13, 12, 1)
ROW_ORDER = (5, 4, 3, 7, 1, 2, 6)


def start_along(axis, me, flips, order, buffer, send, recv):
    for which in order:
        pltpu.make_async_remote_copy(
            src_ref=buffer.at[me],
            dst_ref=buffer.at[me],
            send_sem=send,
            recv_sem=recv,
            device_id={axis: flipped(me, flips, which)},
            device_id_type=MESH,
        ).start()


def wait_slots(buffer, sem):
    slots = buffer.at[pl.ds(0, buffer.shape[0] - 1)]
    pltpu.make_async_copy(slots, slots, sem).wait()


def exclusive_or(first, second, bits):
    total = 0
    for k in range(bits):
        total = total + (1 << k) * lax.rem(first // (1 << k) + second // (1 << k), 2)
    return total


def whole_kernel(
    rows, cols,
    map_hbm, count_hbm, cam_hbm, pt_hbm, res_hbm, partner_hbm, table_hbm,
    tile, update_ref, residual_ref,
    map_smem, count_smem, map_ref, cam_ref, pt_ref, res_ref, partner_ref, rank,
    high, low, own_acc, lane_index, group_index, lhs, acc, weave,
    panel, received, sums, grads, grad_parts, parts, selection,
    first_right, second_right, blocks,
    direction, remainder, answer, row_firsts, col_first, row_second, col_seconds,
    input_sems, panel_send, panel_recv, parts_send, parts_recv,
    first_send, first_recv, second_send, second_recv,
    send_row, recv_row, send_col, recv_col, send_row2, recv_row2, send_col2, recv_col2,
):
    row, col = lax.axis_index("row"), lax.axis_index("col")
    me = row * cols + col
    devices = rows * cols
    row_flips, col_flips = xor_flips(row, 3), xor_flips(col, 4)
    spread_row = functools.partial(start_along, "col", col, col_flips, COL_ORDER)
    spread_col = functools.partial(start_along, "row", row, row_flips, ROW_ORDER)
    scn, points = partner_ref.shape
    chunks = points // LANES
    lines = map_ref.shape[0]
    groups = 8

    inputs = [
        pltpu.make_async_copy(source, target, input_sems.at[k])
        for k, (source, target) in enumerate(
            (
                (map_hbm, map_smem), (count_hbm, count_smem), (table_hbm, map_ref),
                (pt_hbm, pt_ref), (cam_hbm, cam_ref), (res_hbm, res_ref), (partner_hbm, partner_ref),
            )
        )
    ]
    for copy in inputs:
        copy.start()

    barrier = pltpu.get_barrier_semaphore()

    def greet(k, carry):
        other = lax.rem(me + k, devices)
        pl.semaphore_signal(
            barrier, inc=1, device_id=(other // cols, lax.rem(other, cols)), device_id_type=MESH
        )
        return carry

    lax.fori_loop(1, devices, greet, 0)
    own_acc[...] = jnp.zeros_like(own_acc)
    acc[...] = jnp.zeros_like(acc)
    high[pl.ds((VALUES - 1) * scn, scn), :] = jnp.zeros((scn, points), F32)
    low[pl.ds((VALUES - 1) * scn, scn), :] = jnp.zeros((scn, points), F32)
    for copy in inputs:
        copy.wait()

    for s in range(scn):
        here = map_smem[me * scn + s]
        total = jnp.int32(0)
        for t in range(scn):
            if t != s:
                total = total + (map_smem[me * scn + t] < here).astype(jnp.int32)
        rank[s] = total

    def scalars_column(ref, offset, shape):
        line = lax.broadcasted_iota(jnp.int32, shape, 0)
        column = jnp.zeros(shape, jnp.int32)
        for s in range(shape[0]):
            column = jnp.where(line == s, ref[offset + s], column)
        return column

    counts = scalars_column(count_smem, 0, (scn, LANES))

    def chunk(j, carry):
        at = pl.ds(pl.multiple_of(j * LANES, LANES), LANES)
        slot = lax.broadcasted_iota(jnp.int32, (scn, LANES), 1) + j * LANES
        active = (slot < counts).astype(F32)
        values, own = point_chunk(cam_ref, pt_ref, res_ref, active, at)
        for v, value in enumerate(values):
            top = value.astype(BF16).astype(F32)
            high[pl.ds(v * scn, scn), at] = top
            low[pl.ds(v * scn, scn), at] = value - top
        for v, value in enumerate(own):
            own_acc[v] += value
        partner = partner_ref[:, at]
        which = partner & (LANES - 1)
        line = partner >> 7
        position = jnp.zeros((scn, LANES), jnp.int32)
        for h in range(lines):
            table_row = jnp.broadcast_to(map_ref[h : h + 1, :], (scn, LANES))
            position = jnp.where(line == h, jnp.take_along_axis(table_row, which, axis=1), position)
        column = position >> 7
        lane_index[:, at] = ((column >> 3) << 7) | (position & (LANES - 1))
        group_index[:, at] = column & 7
        return carry

    lax.fori_loop(0, chunks, chunk, 0)

    def scatter(s, first, count, buffer):
        group_row = jnp.broadcast_to(group_index[pl.ds(s, 1), :], (groups, points))
        keep = group_row == lax.broadcasted_iota(jnp.int32, (groups, points), 0)
        lane_row = lane_index[pl.ds(s, 1), :]
        onehot = jnp.where(
            lane_row == lax.broadcasted_iota(jnp.int32, (256, points), 0), 1.0, 0.0
        ).astype(BF16)
        for part, source in enumerate((high, low)):
            for v in range(0, count, 2):
                pieces = [
                    jnp.where(
                        keep,
                        jnp.broadcast_to(source[pl.ds((first + v + k) * scn + s, 1), :], (groups, points)),
                        0.0,
                    )
                    for k in range(2)
                ]
                lhs[buffer, pl.ds((part * count + v) * groups, 2 * groups), :] = jnp.concatenate(pieces, axis=0).astype(BF16)
        result = lax.dot_general(
            lhs[buffer, : 2 * count * groups], onehot, (((1,), (1,)), ((), ())), preferred_element_type=F32
        )
        return result[: count * groups] + result[count * groups :]

    first_target = exclusive_or(row, lax.rem(col, rows), 3)

    panel_view = panel.reshape(LINK, rows, 2, 2 * groups, LANES)

    def link_rows(k, carry):
        target = exclusive_or(first_target, k, 3)
        for slot in range(2):
            s = jnp.int32(0)
            for t in range(scn):
                s = jnp.where(rank[t] == target * 2 + slot, t, s)
            result = scatter(s, 0, LINK, slot)
            for x in range(LINK):
                for b in range(2):
                    weave[pl.ds((x * 2 + b) * 2 * groups + slot, groups, stride=2), :] = result[
                        x * groups : (x + 1) * groups, b * LANES : (b + 1) * LANES
                    ]
        panel_view[:, target] = weave[...].reshape(LINK, 2, 2 * groups, LANES).astype(BF16)
        return carry

    def send_rows(k, carry):
        target = exclusive_or(first_target, k, 3)
        for j in COL_ORDER + (0,):
            column = flipped(col, col_flips, j)
            there = target * cols + column

            def send():
                pltpu.make_async_remote_copy(
                    src_ref=panel.at[:, there],
                    dst_ref=received.at[:, me],
                    send_sem=panel_send,
                    recv_sem=panel_recv,
                    device_id=(target, column),
                    device_id_type=MESH,
                ).start()

            if j == 0:
                pl.when(target != row)(send)
            else:
                send()
        return carry

    def link_and_send(k, carry):
        link_rows(k, 0)
        send_rows(k, 0)
        return carry

    link_rows(0, 0)
    pl.semaphore_wait(barrier, devices - 1)
    send_rows(0, 0)

    lanes = lax.broadcasted_iota(jnp.int32, (scn, LANES), 1)
    own_table = jnp.zeros((scn, LANES), F32)
    for v in range(DIAG + 6):
        total = jnp.sum(own_acc[v], axis=1, keepdims=True)
        own_table = jnp.where(lanes == (v if v < DIAG else GRAD_AT + v - DIAG), total, own_table)
    own_table = own_table.T[:SUM_ROWS]
    own_at = scalars_column(map_smem, me * scn, (scn, LANES))
    for column in range(2 * groups):
        spread = (own_at == lanes + column * LANES).astype(F32)
        sums[column // 2, :, (column % 2) * LANES : (column % 2 + 1) * LANES] = lax.dot_general(
            own_table, spread, (((1,), (0,)), ((), ())),
            precision=lax.Precision.HIGHEST, preferred_element_type=F32,
        )

    def other_sums(first, count):
        acc[...] = jnp.zeros_like(acc)

        def pair_sums(pair, carry):
            result = sum(scatter(pair * 2 + k, first, count, k) for k in range(2))
            for b in range(2):
                acc[pl.ds(b * (VALUES - LINK) * groups, count * groups), :] += result[
                    :, b * LANES : (b + 1) * LANES
                ]
            return carry

        lax.fori_loop(0, scn // 2, pair_sums, 0)

    def other_rows(column, count):
        return acc[pl.ds(column // groups * (VALUES - LINK) * groups + column % groups, count, stride=groups), :]

    other_sums(LINK + DIAG, 6)
    zeros = jnp.zeros((3, LANES), F32)
    for column in range(2 * groups):
        lane = slice((column % 2) * LANES, (column % 2 + 1) * LANES)
        grads[column // 2, :, lane] = sums[column // 2, GRAD_AT:, lane] + jnp.concatenate(
            [other_rows(column, 6), zeros[:2]], axis=0
        )

    def start_parts(source, target, send, recv):
        for which in ROW_ORDER:
            there = flipped(row, row_flips, which)
            pltpu.make_async_remote_copy(
                src_ref=source.at[there],
                dst_ref=target.at[row],
                send_sem=send,
                recv_sem=recv,
                device_id={"row": there},
                device_id_type=MESH,
            ).start()

    start_parts(grads, grad_parts, parts_send.at[0], parts_recv.at[0])
    grad_parts[row] = grads[row]
    lax.fori_loop(1, 4, link_and_send, 0)
    wait_slots(grad_parts, parts_recv.at[0])
    first_right[col] = slot_sum(grad_parts)
    spread_row(first_right, first_send, first_recv)
    lax.fori_loop(4, rows, link_and_send, 0)
    received[:, me] = panel[:, me]
    wait_slots(first_right, first_recv)
    second_right[row] = slot_sum(first_right)
    spread_col(second_right, second_send, second_recv)

    other_sums(LINK, DIAG + 1)
    for column in range(2 * groups):
        lane = slice((column % 2) * LANES, (column % 2 + 1) * LANES)
        sums[column // 2, :GRAD_AT, lane] += jnp.concatenate([other_rows(column, DIAG), zeros], axis=0)
    start_parts(sums.at[:, pl.ds(0, GRAD_AT)], parts, parts_send.at[1], parts_recv.at[1])
    parts[row] = sums[row, :GRAD_AT]

    offset = map_ref[...] - row * 256
    inside = (offset >= 0) & (offset < 256)
    lane = lax.broadcasted_iota(jnp.int32, (lines, LANES), 1)
    least = jnp.where(inside, offset, 256)
    for span in (1, 2, 4, 8):
        ahead = pltpu.roll(least, LANES - span, axis=1)
        behind = pltpu.roll(least, span, axis=1)
        least = jnp.minimum(least, jnp.where((lane & span) == 0, ahead, behind))
    later = (offset != least).astype(jnp.int32)
    source = (lax.broadcasted_iota(jnp.int32, (lines, LANES), 0) * 8 + (lane >> 4)) * 2 + later
    place = jnp.where(inside, offset, -1)
    source = jnp.where(inside, source, -1)
    deep = lax.broadcasted_iota(jnp.int32, (256, LANES), 0)
    chosen = jnp.zeros((256, 256), F32)
    for h in range(lines):
        place_hot = jnp.where(place[h : h + 1] == deep, 1.0, 0.0).astype(BF16)
        source_hot = jnp.where(source[h : h + 1] == deep, 1.0, 0.0).astype(BF16)
        chosen = chosen + lax.dot_general(
            place_hot, source_hot, (((1,), (1,)), ((), ())), preferred_element_type=F32
        )
    selection[...] = chosen.astype(BF16)

    landed = received.at[:, pl.ds(0, devices - 1)]
    pltpu.make_async_copy(landed, landed, panel_recv).wait()
    received_view = received.reshape(LINK, 2 * devices, LANES)

    def select(block, carry):
        for k in range(6):
            x = (block * 6 + k) * 2
            pair = jnp.concatenate([received_view[x], received_view[x + 1]], axis=1)
            chosen_rows = jnp.dot(selection[...], pair, preferred_element_type=F32).astype(BF16)
            tile[x] = chosen_rows[:, :LANES]
            tile[x + 1] = chosen_rows[:, LANES:]
        return carry

    lax.fori_loop(0, LINK // 12, select, 0)

    wait_slots(second_right, second_recv)
    start = second_right[...]
    direction[...] = start
    remainder[...] = start
    answer[...] = jnp.zeros_like(answer)

    def inner_product(first, second):
        total = first[0] * second[0]
        for r in range(1, rows):
            total = total + first[r] * second[r]
        return jnp.sum(jnp.sum(total, axis=0, keepdims=True), axis=1, keepdims=True)

    norm_start = inner_product(start, start)
    wait_slots(parts, parts_recv.at[1])
    total = slot_sum(parts)
    line = lax.broadcasted_iota(jnp.int32, (8, 256), 0)
    for y in range(6):
        block = jnp.zeros((8, 256), F32)
        for x in range(6):
            v = pair_index(x, y)
            block = jnp.where(line == x, jnp.broadcast_to(total[v : v + 1], (8, 256)), block)
        blocks[y] = block

    def iteration(step, norm_now):
        parity = lax.rem(step, 2)
        row_first, col_second = row_firsts.at[parity], col_seconds.at[parity]
        rows_part = direction[row]
        cols_part = direction[col // 2, :, pl.ds(pl.multiple_of(lax.rem(col, 2) * LANES, LANES), LANES)]
        row_terms, col_terms = three_terms(rows_part), three_terms(cols_part)
        col_lhs = [row_masked(col_terms, y) for y in range(6)]
        row_lhs = [row_masked(row_terms, x) for x in range(6)]
        line_rows = lax.broadcasted_iota(jnp.int32, (8, 256), 0)
        line_cols = lax.broadcasted_iota(jnp.int32, (8, LANES), 0)
        forward = jnp.zeros((8, 256), F32)
        for y in range(6):
            forward = forward + blocks[y] * jnp.broadcast_to(rows_part[y : y + 1], (8, 256))
        for x in range(6):
            total = None
            for y in range(6):
                part = lax.dot_general(
                    col_lhs[y], tile[x * 6 + y], (((1,), (1,)), ((), ())), preferred_element_type=F32
                )
                total = part if total is None else total + part
            forward = forward + jnp.where(line_rows == x, jnp.sum(total, axis=0, keepdims=True), 0.0)
        row_first[col] = forward
        spread_row(row_first, send_row.at[parity], recv_row.at[parity])
        backward = jnp.zeros((8, LANES), F32)
        for y in range(6):
            total = None
            for x in range(6):
                part = jnp.dot(row_lhs[x], tile[x * 6 + y], preferred_element_type=F32)
                total = part if total is None else total + part
            backward = backward + jnp.where(line_cols == y, jnp.sum(total, axis=0, keepdims=True), 0.0)
        col_first[row] = backward
        spread_col(col_first, send_col, recv_col)
        wait_slots(col_first, recv_col)
        col_second[col] = slot_sum(col_first)
        spread_row(col_second, send_col2.at[parity], recv_col2.at[parity])
        wait_slots(row_first, recv_row.at[parity])
        row_second[row] = slot_sum(row_first)
        spread_col(row_second, send_row2, recv_row2)
        wait_slots(row_second, recv_row2)
        wait_slots(col_second, recv_col2.at[parity])
        wait_slots(row_first, send_row.at[parity])
        wait_slots(col_first, send_col)
        wait_slots(row_second, send_row2)
        wait_slots(col_second, send_col2.at[parity])
        held = direction[...]
        image = CAMERA_DAMPING * held + row_second[...]
        back = jnp.stack(
            [jnp.concatenate([col_second[2 * r], col_second[2 * r + 1]], axis=1) for r in range(rows)], axis=0
        )
        image = image + back
        step_size = norm_now / inner_product(held, image)
        answer[...] = answer[...] + step_size[None] * held
        left = remainder[...] - step_size[None] * image
        remainder[...] = left
        norm_next = inner_product(left, left)
        direction[...] = left + (norm_next / norm_now)[None] * held
        return norm_next

    lax.fori_loop(0, ITERS, iteration, norm_start)
    update_ref[...] = answer[row][:6]
    residual_ref[...] = remainder[row][:6]
    sent = panel.at[:, pl.ds(0, devices - 1)]
    pltpu.make_async_copy(sent, sent, panel_send).wait()
    wait_slots(grad_parts, parts_send.at[0])
    wait_slots(parts, parts_send.at[1])
    wait_slots(first_right, first_send)
    wait_slots(second_right, second_send)


def store_kernel(*refs):
    count = len(refs) // 2
    sems = refs[-1]
    copies = [pltpu.make_async_copy(refs[k], refs[count + k], sems.at[k]) for k in range(count)]
    for copy in copies:
        copy.start()
    for copy in copies:
        copy.wait()


def store(arrays):
    return pl.pallas_call(
        store_kernel,
        in_specs=[pl.BlockSpec(memory_space=pltpu.VMEM)] * len(arrays),
        out_specs=[pl.BlockSpec(memory_space=pltpu.HBM)] * len(arrays),
        out_shape=[jax.ShapeDtypeStruct(array.shape, array.dtype) for array in arrays],
        scratch_shapes=[pltpu.SemaphoreType.DMA((len(arrays),))],
        compiler_params=pltpu.CompilerParams(vmem_limit_bytes=8 * 1024 * 1024),
        name="store",
    )(*arrays)


def shards(cam_jac, pt_jac, resid, partner, count, tile_map):
    rows, cols = lax.axis_size("row"), lax.axis_size("col")
    scn, points = partner.shape
    devices = rows * cols
    groups = 8
    dma = pltpu.SemaphoreType.DMA
    vmem = pltpu.VMEM
    vmem_spec = pl.BlockSpec(memory_space=pltpu.VMEM)
    hbm_spec = pl.BlockSpec(memory_space=pltpu.HBM)
    coupling, update, residual = pl.pallas_call(
        functools.partial(whole_kernel, rows, cols),
        in_specs=[hbm_spec] * 7,
        out_specs=[vmem_spec] * 3,
        out_shape=[
            jax.ShapeDtypeStruct((LINK, 256, LANES), BF16),
            jax.ShapeDtypeStruct((6, 256), F32),
            jax.ShapeDtypeStruct((6, 256), F32),
        ],
        scratch_shapes=[
            pltpu.SMEM(tile_map.shape, jnp.int32),
            pltpu.SMEM(count.shape, jnp.int32),
            vmem((tile_map.shape[0] // LANES, LANES), jnp.int32),
            vmem(cam_jac.shape, BF16),
            vmem(pt_jac.shape, BF16),
            vmem(resid.shape, BF16),
            vmem(partner.shape, jnp.int32),
            pltpu.SMEM((scn,), jnp.int32),
            vmem((VALUES * scn, points), F32),
            vmem((VALUES * scn, points), F32),
            vmem((DIAG + 6, scn, LANES), F32),
            vmem((scn, points), jnp.int32),
            vmem((scn, points), jnp.int32),
            vmem((2, 2 * LINK * groups, points), BF16),
            vmem((2 * (VALUES - LINK) * groups, LANES), F32),
            vmem((LINK * 2 * 2 * groups, LANES), F32),
            vmem((LINK, devices, 2, LANES), BF16),
            vmem((LINK, devices, 2, LANES), BF16),
            vmem((rows, SUM_ROWS, 256), F32),
            vmem((rows, 8, 256), F32),
            vmem((rows, 8, 256), F32),
            vmem((rows, GRAD_AT, 256), F32),
            vmem((256, 256), BF16),
            vmem((cols, 8, 256), F32),
            vmem((rows, 8, 256), F32),
            vmem((6, 8, 256), F32),
            vmem((rows, 8, 256), F32),
            vmem((rows, 8, 256), F32),
            vmem((rows, 8, 256), F32),
            vmem((2, cols, 8, 256), F32),
            vmem((rows, 8, LANES), F32),
            vmem((rows, 8, 256), F32),
            vmem((2, cols, 8, LANES), F32),
            dma((7,)), dma, dma, dma((2,)), dma((2,)),
            dma, dma, dma, dma,
            dma((2,)), dma((2,)), dma, dma, dma, dma, dma((2,)), dma((2,)),
        ],
        compiler_params=pltpu.CompilerParams(
            collective_id=0, has_side_effects=True, vmem_limit_bytes=48 * 1024 * 1024
        ),
        name="bundle",
    )(
        *(
            pltpu.with_memory_space_constraint(array, pltpu.HBM)
            for array in (tile_map, count, cam_jac, pt_jac, resid, partner, tile_map.reshape(-1, LANES))
        )
    )
    coupling, update, residual = store([coupling, update, residual])
    return coupling.reshape(6, 6, 256, LANES), update, residual


def solution(mesh):
    return jax.shard_map(
        shards,
        mesh=mesh,
        in_specs=(
            P(None, None, None, ("row", "col"), None),
            P(None, None, None, ("row", "col"), None),
            P(None, None, ("row", "col"), None),
            P(("row", "col"), None),
            P(("row", "col")),
            P(),
        ),
        out_specs=(P(None, None, "row", "col"), P(None, "row"), P(None, "row")),
        check_vma=False,
    )
```

```python
import functools

import jax
import jax.numpy as jnp
from jax import lax
from jax.experimental import pallas as pl
from jax.experimental.pallas import tpu as pltpu
from jax.sharding import PartitionSpec as P

ITERS = 3
CAMERA_DAMPING = 1.0
POINT_DAMPING = 1.0

F32 = jnp.float32
BF16 = jnp.bfloat16
MESH = pl.DeviceIdType.MESH
LANES = 128

LINK = 36
PAIRS = [(x, y) for x in range(6) for y in range(x, 6)]
DIAG = len(PAIRS)
VALUES = 64
GRAD_AT = 24
SUM_ROWS = 32


def pair_index(x, y):
    return PAIRS.index((min(x, y), max(x, y)))


def dot3(first, second):
    total = first[0] * second[0]
    for k in range(1, len(first)):
        total = total + first[k] * second[k]
    return total


def point_chunk(cam_ref, pt_ref, res_ref, active, at):
    def cam(side, i):
        return [cam_ref[side, i, x, :, at].astype(F32) for x in range(6)]

    pa = [[pt_ref[0, i, k, :, at].astype(F32) for k in range(3)] for i in range(2)]
    pb = [[pt_ref[1, i, k, :, at].astype(F32) for k in range(3)] for i in range(2)]
    ea = [res_ref[0, i, :, at].astype(F32) for i in range(2)]
    eb = [res_ref[1, i, :, at].astype(F32) for i in range(2)]

    def hess(m, n):
        return pa[0][m] * pa[0][n] + pa[1][m] * pa[1][n] + (pb[0][m] * pb[0][n] + pb[1][m] * pb[1][n])

    v00, v11, v22 = (hess(k, k) + POINT_DAMPING for k in range(3))
    v01, v02, v12 = hess(0, 1), hess(0, 2), hess(1, 2)
    c00 = v11 * v22 - v12 * v12
    c01 = v02 * v12 - v01 * v22
    c02 = v01 * v12 - v02 * v11
    c11 = v00 * v22 - v02 * v02
    c12 = v01 * v02 - v00 * v12
    c22 = v00 * v11 - v01 * v01
    det = v00 * c00 + v01 * c01 + v02 * c02
    scale = 1.0 / det
    i00, i01, i02 = c00 * scale, c01 * scale, c02 * scale
    i11, i12, i22 = c11 * scale, c12 * scale, c22 * scale
    inv = [[i00, i01, i02], [i01, i11, i12], [i02, i12, i22]]
    q = [-(pa[0][k] * ea[0] + pa[1][k] * ea[1] + (pb[0][k] * eb[0] + pb[1][k] * eb[1])) for k in range(3)]
    pav = [[dot3(pa[i], inv[k]) for k in range(3)] for i in range(2)]
    pbv = [[dot3(pb[i], inv[k]) for k in range(3)] for i in range(2)]

    def schur(pv, p):
        n00 = (1.0 - dot3(pv[0], p[0])) * active
        n01 = -dot3(pv[0], p[1]) * active
        n11 = (1.0 - dot3(pv[1], p[1])) * active
        return [[n00, n01], [n01, n11]]

    naa, nbb = schur(pav, pa), schur(pbv, pb)
    mab = [[-dot3(pav[i], pb[j]) * active for j in range(2)] for i in range(2)]
    ga = [-(ea[i] + dot3(pav[i], q)) * active for i in range(2)]
    gb = [-(eb[i] + dot3(pbv[i], q)) * active for i in range(2)]
    ja = [cam(0, 0), cam(0, 1)]
    jb = [cam(1, 0), cam(1, 1)]

    def quad(left, middle, right, pairs):
        half = [[middle[i][0] * right[0][y] + middle[i][1] * right[1][y] for y in range(6)] for i in range(2)]
        return [left[0][x] * half[0][y] + left[1][x] * half[1][y] for x, y in pairs]

    link = quad(ja, mab, jb, [(x, y) for x in range(6) for y in range(6)])
    diag_other = quad(jb, nbb, jb, PAIRS)
    grad_other = [jb[0][x] * gb[0] + jb[1][x] * gb[1] for x in range(6)]
    diag_own = quad(ja, naa, ja, PAIRS)
    grad_own = [ja[0][x] * ga[0] + ja[1][x] * ga[1] for x in range(6)]
    return link + diag_other + grad_other, diag_own + grad_own


def slot_sum(buffer):
    total = buffer[0]
    for k in range(1, buffer.shape[0]):
        total = total + buffer[k]
    return total


def three_terms(value):
    first = value.astype(BF16)
    rest = value - first.astype(F32)
    second = rest.astype(BF16)
    third = (rest - second.astype(F32)).astype(BF16)
    return jnp.concatenate([first.astype(F32), second.astype(F32), third.astype(F32)], axis=0)


def row_masked(stacked, which):
    line = lax.broadcasted_iota(jnp.int32, stacked.shape, 0) & 7
    return jnp.where(line == which, stacked, 0.0).astype(BF16)


def xor_flips(index, bits):
    return [(1 << k) * (1 - 2 * lax.rem(index // (1 << k), 2)) for k in range(bits)]


def flipped(index, flips, which):
    for k, flip in enumerate(flips):
        if which >> k & 1:
            index = index + flip
    return index


COL_ORDER = (11, 10, 9, 8, 7, 6, 15, 14, 3, 2, 5, 4, 13, 12, 1)
ROW_ORDER = (5, 4, 3, 7, 1, 2, 6)


def start_along(axis, me, flips, order, buffer, send, recv):
    for which in order:
        pltpu.make_async_remote_copy(
            src_ref=buffer.at[me],
            dst_ref=buffer.at[me],
            send_sem=send,
            recv_sem=recv,
            device_id={axis: flipped(me, flips, which)},
            device_id_type=MESH,
        ).start()


def wait_slots(buffer, sem):
    slots = buffer.at[pl.ds(0, buffer.shape[0] - 1)]
    pltpu.make_async_copy(slots, slots, sem).wait()


def exclusive_or(first, second, bits):
    total = 0
    for k in range(bits):
        total = total + (1 << k) * lax.rem(first // (1 << k) + second // (1 << k), 2)
    return total


def whole_kernel(
    rows, cols,
    map_hbm, count_hbm, cam_hbm, pt_hbm, res_hbm, partner_hbm, table_hbm,
    tile, update_ref, residual_ref,
    map_smem, count_smem, map_ref, cam_ref, pt_ref, res_ref, partner_ref, rank,
    high, low, own_acc, lane_index, group_index, lhs, acc, weave,
    panel, received, sums, grads, grad_parts, parts, selection,
    first_right, second_right, blocks,
    direction, remainder, answer, row_firsts, col_first, row_second, col_seconds,
    input_sems, panel_send, panel_recv, parts_send, parts_recv,
    first_send, first_recv, second_send, second_recv,
    send_row, recv_row, send_col, recv_col, send_row2, recv_row2, send_col2, recv_col2,
):
    row, col = lax.axis_index("row"), lax.axis_index("col")
    me = row * cols + col
    devices = rows * cols
    row_flips, col_flips = xor_flips(row, 3), xor_flips(col, 4)
    spread_row = functools.partial(start_along, "col", col, col_flips, COL_ORDER)
    spread_col = functools.partial(start_along, "row", row, row_flips, ROW_ORDER)
    scn, points = partner_ref.shape
    chunks = points // LANES
    lines = map_ref.shape[0]
    groups = 8

    inputs = [
        pltpu.make_async_copy(source, target, input_sems.at[k])
        for k, (source, target) in enumerate(
            (
                (map_hbm, map_smem), (count_hbm, count_smem), (table_hbm, map_ref),
                (pt_hbm, pt_ref), (cam_hbm, cam_ref), (res_hbm, res_ref), (partner_hbm, partner_ref),
            )
        )
    ]
    for copy in inputs:
        copy.start()

    barrier = pltpu.get_barrier_semaphore()

    def greet(k, carry):
        target = exclusive_or(row, k, 3)
        for j in COL_ORDER + (0,):

            def signal(column=flipped(col, col_flips, j)):
                pl.semaphore_signal(barrier, inc=1, device_id=(target, column), device_id_type=MESH)

            if j == 0:
                pl.when(k > 0)(signal)
            else:
                signal()
        return carry

    lax.fori_loop(0, rows, greet, 0)
    own_acc[...] = jnp.zeros_like(own_acc)
    acc[...] = jnp.zeros_like(acc)
    high[pl.ds((VALUES - 1) * scn, scn), :] = jnp.zeros((scn, points), F32)
    low[pl.ds((VALUES - 1) * scn, scn), :] = jnp.zeros((scn, points), F32)
    for copy in inputs:
        copy.wait()

    for s in range(scn):
        here = map_smem[me * scn + s]
        total = jnp.int32(0)
        for t in range(scn):
            if t != s:
                total = total + (map_smem[me * scn + t] < here).astype(jnp.int32)
        rank[s] = total

    def scalars_column(ref, offset, shape):
        line = lax.broadcasted_iota(jnp.int32, shape, 0)
        column = jnp.zeros(shape, jnp.int32)
        for s in range(shape[0]):
            column = jnp.where(line == s, ref[offset + s], column)
        return column

    counts = scalars_column(count_smem, 0, (scn, LANES))

    def chunk(j, carry):
        at = pl.ds(pl.multiple_of(j * LANES, LANES), LANES)
        slot = lax.broadcasted_iota(jnp.int32, (scn, LANES), 1) + j * LANES
        active = (slot < counts).astype(F32)
        values, own = point_chunk(cam_ref, pt_ref, res_ref, active, at)
        for v, value in enumerate(values):
            top = value.astype(BF16).astype(F32)
            high[pl.ds(v * scn, scn), at] = top
            low[pl.ds(v * scn, scn), at] = value - top
        for v, value in enumerate(own):
            own_acc[v] += value
        partner = partner_ref[:, at]
        which = partner & (LANES - 1)
        line = partner >> 7
        position = jnp.zeros((scn, LANES), jnp.int32)
        for h in range(lines):
            table_row = jnp.broadcast_to(map_ref[h : h + 1, :], (scn, LANES))
            position = jnp.where(line == h, jnp.take_along_axis(table_row, which, axis=1), position)
        column = position >> 7
        lane_index[:, at] = ((column >> 3) << 7) | (position & (LANES - 1))
        group_index[:, at] = column & 7
        return carry

    lax.fori_loop(0, chunks, chunk, 0)

    def scatter(s, first, count, buffer):
        group_row = jnp.broadcast_to(group_index[pl.ds(s, 1), :], (groups, points))
        keep = group_row == lax.broadcasted_iota(jnp.int32, (groups, points), 0)
        lane_row = lane_index[pl.ds(s, 1), :]
        onehot = jnp.where(
            lane_row == lax.broadcasted_iota(jnp.int32, (256, points), 0), 1.0, 0.0
        ).astype(BF16)
        for part, source in enumerate((high, low)):
            for v in range(0, count, 2):
                pieces = [
                    jnp.where(
                        keep,
                        jnp.broadcast_to(source[pl.ds((first + v + k) * scn + s, 1), :], (groups, points)),
                        0.0,
                    )
                    for k in range(2)
                ]
                lhs[buffer, pl.ds((part * count + v) * groups, 2 * groups), :] = jnp.concatenate(pieces, axis=0).astype(BF16)
        result = lax.dot_general(
            lhs[buffer, : 2 * count * groups], onehot, (((1,), (1,)), ((), ())), preferred_element_type=F32
        )
        return result[: count * groups] + result[count * groups :]

    first_target = exclusive_or(row, lax.rem(col, rows), 3)

    panel_view = panel.reshape(LINK, rows, 2, 2 * groups, LANES)

    def link_rows(k, carry):
        target = exclusive_or(first_target, k, 3)
        for slot in range(2):
            s = jnp.int32(0)
            for t in range(scn):
                s = jnp.where(rank[t] == target * 2 + slot, t, s)
            result = scatter(s, 0, LINK, slot)
            for x in range(LINK):
                for b in range(2):
                    weave[pl.ds((x * 2 + b) * 2 * groups + slot, groups, stride=2), :] = result[
                        x * groups : (x + 1) * groups, b * LANES : (b + 1) * LANES
                    ]
        panel_view[:, target] = weave[...].reshape(LINK, 2, 2 * groups, LANES).astype(BF16)
        return carry

    def send_rows(k, carry):
        target = exclusive_or(first_target, k, 3)
        for j in COL_ORDER + (0,):
            column = flipped(col, col_flips, j)
            there = target * cols + column

            def send():
                pltpu.make_async_remote_copy(
                    src_ref=panel.at[:, there],
                    dst_ref=received.at[:, me],
                    send_sem=panel_send,
                    recv_sem=panel_recv,
                    device_id=(target, column),
                    device_id_type=MESH,
                ).start()

            if j == 0:
                pl.when(target != row)(send)
            else:
                send()
        return carry

    def link_and_send(k, carry):
        link_rows(k, 0)
        send_rows(k, 0)
        return carry

    link_rows(0, 0)
    pl.semaphore_wait(barrier, devices - 1)
    send_rows(0, 0)

    lanes = lax.broadcasted_iota(jnp.int32, (scn, LANES), 1)
    own_table = jnp.zeros((scn, LANES), F32)
    for v in range(DIAG + 6):
        total = jnp.sum(own_acc[v], axis=1, keepdims=True)
        own_table = jnp.where(lanes == (v if v < DIAG else GRAD_AT + v - DIAG), total, own_table)
    own_table = own_table.T[:SUM_ROWS]
    own_at = scalars_column(map_smem, me * scn, (scn, LANES))
    for column in range(2 * groups):
        spread = (own_at == lanes + column * LANES).astype(F32)
        sums[column // 2, :, (column % 2) * LANES : (column % 2 + 1) * LANES] = lax.dot_general(
            own_table, spread, (((1,), (0,)), ((), ())),
            precision=lax.Precision.HIGHEST, preferred_element_type=F32,
        )

    def other_sums(first, count):
        acc[...] = jnp.zeros_like(acc)

        def pair_sums(pair, carry):
            result = sum(scatter(pair * 2 + k, first, count, k) for k in range(2))
            for b in range(2):
                acc[pl.ds(b * (VALUES - LINK) * groups, count * groups), :] += result[
                    :, b * LANES : (b + 1) * LANES
                ]
            return carry

        lax.fori_loop(0, scn // 2, pair_sums, 0)

    def other_rows(column, count):
        return acc[pl.ds(column // groups * (VALUES - LINK) * groups + column % groups, count, stride=groups), :]

    other_sums(LINK + DIAG, 6)
    zeros = jnp.zeros((3, LANES), F32)
    for column in range(2 * groups):
        lane = slice((column % 2) * LANES, (column % 2 + 1) * LANES)
        grads[column // 2, :, lane] = sums[column // 2, GRAD_AT:, lane] + jnp.concatenate(
            [other_rows(column, 6), zeros[:2]], axis=0
        )

    def start_parts(source, target, send, recv):
        for which in ROW_ORDER:
            there = flipped(row, row_flips, which)
            pltpu.make_async_remote_copy(
                src_ref=source.at[there],
                dst_ref=target.at[row],
                send_sem=send,
                recv_sem=recv,
                device_id={"row": there},
                device_id_type=MESH,
            ).start()

    start_parts(grads, grad_parts, parts_send.at[0], parts_recv.at[0])
    grad_parts[row] = grads[row]
    lax.fori_loop(1, 4, link_and_send, 0)
    wait_slots(grad_parts, parts_recv.at[0])
    first_right[col] = slot_sum(grad_parts)
    spread_row(first_right, first_send, first_recv)
    lax.fori_loop(4, rows, link_and_send, 0)
    received[:, me] = panel[:, me]
    wait_slots(first_right, first_recv)
    second_right[row] = slot_sum(first_right)
    spread_col(second_right, second_send, second_recv)

    other_sums(LINK, DIAG + 1)
    for column in range(2 * groups):
        lane = slice((column % 2) * LANES, (column % 2 + 1) * LANES)
        sums[column // 2, :GRAD_AT, lane] += jnp.concatenate([other_rows(column, DIAG), zeros], axis=0)
    start_parts(sums.at[:, pl.ds(0, GRAD_AT)], parts, parts_send.at[1], parts_recv.at[1])
    parts[row] = sums[row, :GRAD_AT]

    offset = map_ref[...] - row * 256
    inside = (offset >= 0) & (offset < 256)
    lane = lax.broadcasted_iota(jnp.int32, (lines, LANES), 1)
    least = jnp.where(inside, offset, 256)
    for span in (1, 2, 4, 8):
        ahead = pltpu.roll(least, LANES - span, axis=1)
        behind = pltpu.roll(least, span, axis=1)
        least = jnp.minimum(least, jnp.where((lane & span) == 0, ahead, behind))
    later = (offset != least).astype(jnp.int32)
    source = (lax.broadcasted_iota(jnp.int32, (lines, LANES), 0) * 8 + (lane >> 4)) * 2 + later
    place = jnp.where(inside, offset, -1)
    source = jnp.where(inside, source, -1)
    deep = lax.broadcasted_iota(jnp.int32, (256, LANES), 0)
    chosen = jnp.zeros((256, 256), F32)
    for h in range(lines):
        place_hot = jnp.where(place[h : h + 1] == deep, 1.0, 0.0).astype(BF16)
        source_hot = jnp.where(source[h : h + 1] == deep, 1.0, 0.0).astype(BF16)
        chosen = chosen + lax.dot_general(
            place_hot, source_hot, (((1,), (1,)), ((), ())), preferred_element_type=F32
        )
    selection[...] = chosen.astype(BF16)

    landed = received.at[:, pl.ds(0, devices - 1)]
    pltpu.make_async_copy(landed, landed, panel_recv).wait()
    received_view = received.reshape(LINK, 2 * devices, LANES)

    def select(block, carry):
        for k in range(6):
            x = (block * 6 + k) * 2
            pair = jnp.concatenate([received_view[x], received_view[x + 1]], axis=1)
            chosen_rows = jnp.dot(selection[...], pair, preferred_element_type=F32).astype(BF16)
            tile[x] = chosen_rows[:, :LANES]
            tile[x + 1] = chosen_rows[:, LANES:]
        return carry

    lax.fori_loop(0, LINK // 12, select, 0)

    wait_slots(second_right, second_recv)
    start = second_right[...]
    direction[...] = start
    remainder[...] = start
    answer[...] = jnp.zeros_like(answer)

    def inner_product(first, second):
        total = first[0] * second[0]
        for r in range(1, rows):
            total = total + first[r] * second[r]
        return jnp.sum(jnp.sum(total, axis=0, keepdims=True), axis=1, keepdims=True)

    norm_start = inner_product(start, start)
    wait_slots(parts, parts_recv.at[1])
    total = slot_sum(parts)
    line = lax.broadcasted_iota(jnp.int32, (8, 256), 0)
    for y in range(6):
        block = jnp.zeros((8, 256), F32)
        for x in range(6):
            v = pair_index(x, y)
            block = jnp.where(line == x, jnp.broadcast_to(total[v : v + 1], (8, 256)), block)
        blocks[y] = block

    def iteration(step, norm_now):
        parity = lax.rem(step, 2)
        row_first, col_second = row_firsts.at[parity], col_seconds.at[parity]
        rows_part = direction[row]
        cols_part = direction[col // 2, :, pl.ds(pl.multiple_of(lax.rem(col, 2) * LANES, LANES), LANES)]
        row_terms, col_terms = three_terms(rows_part), three_terms(cols_part)
        col_lhs = [row_masked(col_terms, y) for y in range(6)]
        row_lhs = [row_masked(row_terms, x) for x in range(6)]
        line_rows = lax.broadcasted_iota(jnp.int32, (8, 256), 0)
        line_cols = lax.broadcasted_iota(jnp.int32, (8, LANES), 0)
        forward = jnp.zeros((8, 256), F32)
        for y in range(6):
            forward = forward + blocks[y] * jnp.broadcast_to(rows_part[y : y + 1], (8, 256))
        for x in range(6):
            wide = jnp.concatenate([tile[x * 6 + y] for y in range(6)], axis=1)
            total = lax.dot_general(
                jnp.concatenate(col_lhs, axis=1), wide, (((1,), (1,)), ((), ())), preferred_element_type=F32
            )
            forward = forward + jnp.where(line_rows == x, jnp.sum(total, axis=0, keepdims=True), 0.0)
        row_first[col] = forward
        spread_row(row_first, send_row.at[parity], recv_row.at[parity])
        backward = jnp.zeros((8, LANES), F32)
        for y in range(6):
            total = None
            for x in range(6):
                part = jnp.dot(row_lhs[x], tile[x * 6 + y], preferred_element_type=F32)
                total = part if total is None else total + part
            backward = backward + jnp.where(line_cols == y, jnp.sum(total, axis=0, keepdims=True), 0.0)
        col_first[row] = backward
        spread_col(col_first, send_col, recv_col)
        wait_slots(col_first, recv_col)
        col_second[col] = slot_sum(col_first)
        spread_row(col_second, send_col2.at[parity], recv_col2.at[parity])
        wait_slots(row_first, recv_row.at[parity])
        row_second[row] = slot_sum(row_first)
        spread_col(row_second, send_row2, recv_row2)
        wait_slots(row_second, recv_row2)
        wait_slots(col_second, recv_col2.at[parity])
        wait_slots(row_first, send_row.at[parity])
        wait_slots(col_first, send_col)
        wait_slots(row_second, send_row2)
        wait_slots(col_second, send_col2.at[parity])
        held = direction[...]
        image = CAMERA_DAMPING * held + row_second[...]
        back = jnp.stack(
            [jnp.concatenate([col_second[2 * r], col_second[2 * r + 1]], axis=1) for r in range(rows)], axis=0
        )
        image = image + back
        step_size = norm_now / inner_product(held, image)
        answer[...] = answer[...] + step_size[None] * held
        left = remainder[...] - step_size[None] * image
        remainder[...] = left
        norm_next = inner_product(left, left)
        direction[...] = left + (norm_next / norm_now)[None] * held
        return norm_next

    lax.fori_loop(0, ITERS, iteration, norm_start)
    update_ref[...] = answer[row][:6]
    residual_ref[...] = remainder[row][:6]
    sent = panel.at[:, pl.ds(0, devices - 1)]
    pltpu.make_async_copy(sent, sent, panel_send).wait()
    wait_slots(grad_parts, parts_send.at[0])
    wait_slots(parts, parts_send.at[1])
    wait_slots(first_right, first_send)
    wait_slots(second_right, second_send)


def store_kernel(*refs):
    count = len(refs) // 2
    sems = refs[-1]
    copies = [pltpu.make_async_copy(refs[k], refs[count + k], sems.at[k]) for k in range(count)]
    for copy in copies:
        copy.start()
    for copy in copies:
        copy.wait()


def store(arrays):
    return pl.pallas_call(
        store_kernel,
        in_specs=[pl.BlockSpec(memory_space=pltpu.VMEM)] * len(arrays),
        out_specs=[pl.BlockSpec(memory_space=pltpu.HBM)] * len(arrays),
        out_shape=[jax.ShapeDtypeStruct(array.shape, array.dtype) for array in arrays],
        scratch_shapes=[pltpu.SemaphoreType.DMA((len(arrays),))],
        compiler_params=pltpu.CompilerParams(vmem_limit_bytes=8 * 1024 * 1024),
        name="store",
    )(*arrays)


def shards(cam_jac, pt_jac, resid, partner, count, tile_map):
    rows, cols = lax.axis_size("row"), lax.axis_size("col")
    scn, points = partner.shape
    devices = rows * cols
    groups = 8
    dma = pltpu.SemaphoreType.DMA
    vmem = pltpu.VMEM
    vmem_spec = pl.BlockSpec(memory_space=pltpu.VMEM)
    hbm_spec = pl.BlockSpec(memory_space=pltpu.HBM)
    coupling, update, residual = pl.pallas_call(
        functools.partial(whole_kernel, rows, cols),
        in_specs=[hbm_spec] * 7,
        out_specs=[vmem_spec] * 3,
        out_shape=[
            jax.ShapeDtypeStruct((LINK, 256, LANES), BF16),
            jax.ShapeDtypeStruct((6, 256), F32),
            jax.ShapeDtypeStruct((6, 256), F32),
        ],
        scratch_shapes=[
            pltpu.SMEM(tile_map.shape, jnp.int32),
            pltpu.SMEM(count.shape, jnp.int32),
            vmem((tile_map.shape[0] // LANES, LANES), jnp.int32),
            vmem(cam_jac.shape, BF16),
            vmem(pt_jac.shape, BF16),
            vmem(resid.shape, BF16),
            vmem(partner.shape, jnp.int32),
            pltpu.SMEM((scn,), jnp.int32),
            vmem((VALUES * scn, points), F32),
            vmem((VALUES * scn, points), F32),
            vmem((DIAG + 6, scn, LANES), F32),
            vmem((scn, points), jnp.int32),
            vmem((scn, points), jnp.int32),
            vmem((2, 2 * LINK * groups, points), BF16),
            vmem((2 * (VALUES - LINK) * groups, LANES), F32),
            vmem((LINK * 2 * 2 * groups, LANES), F32),
            vmem((LINK, devices, 2, LANES), BF16),
            vmem((LINK, devices, 2, LANES), BF16),
            vmem((rows, SUM_ROWS, 256), F32),
            vmem((rows, 8, 256), F32),
            vmem((rows, 8, 256), F32),
            vmem((rows, GRAD_AT, 256), F32),
            vmem((256, 256), BF16),
            vmem((cols, 8, 256), F32),
            vmem((rows, 8, 256), F32),
            vmem((6, 8, 256), F32),
            vmem((rows, 8, 256), F32),
            vmem((rows, 8, 256), F32),
            vmem((rows, 8, 256), F32),
            vmem((2, cols, 8, 256), F32),
            vmem((rows, 8, LANES), F32),
            vmem((rows, 8, 256), F32),
            vmem((2, cols, 8, LANES), F32),
            dma((7,)), dma, dma, dma((2,)), dma((2,)),
            dma, dma, dma, dma,
            dma((2,)), dma((2,)), dma, dma, dma, dma, dma((2,)), dma((2,)),
        ],
        compiler_params=pltpu.CompilerParams(
            collective_id=0, has_side_effects=True, vmem_limit_bytes=48 * 1024 * 1024
        ),
        name="bundle",
    )(
        *(
            pltpu.with_memory_space_constraint(array, pltpu.HBM)
            for array in (tile_map, count, cam_jac, pt_jac, resid, partner, tile_map.reshape(-1, LANES))
        )
    )
    coupling, update, residual = store([coupling, update, residual])
    return coupling.reshape(6, 6, 256, LANES), update, residual


def solution(mesh):
    return jax.shard_map(
        shards,
        mesh=mesh,
        in_specs=(
            P(None, None, None, ("row", "col"), None),
            P(None, None, None, ("row", "col"), None),
            P(None, None, ("row", "col"), None),
            P(("row", "col"), None),
            P(("row", "col")),
            P(),
        ),
        out_specs=(P(None, None, "row", "col"), P(None, "row"), P(None, "row")),
        check_vma=False,
    )
```

```python
import functools

import jax
import jax.numpy as jnp
from jax import lax
from jax.experimental import pallas as pl
from jax.experimental.pallas import tpu as pltpu
from jax.sharding import PartitionSpec as P

ITERS = 3
CAMERA_DAMPING = 1.0
POINT_DAMPING = 1.0

F32 = jnp.float32
BF16 = jnp.bfloat16
MESH = pl.DeviceIdType.MESH
LANES = 128

LINK = 36
PAIRS = [(x, y) for x in range(6) for y in range(x, 6)]
DIAG = len(PAIRS)
VALUES = 64
GRAD_AT = 24
SUM_ROWS = 32


def pair_index(x, y):
    return PAIRS.index((min(x, y), max(x, y)))


def dot3(first, second):
    total = first[0] * second[0]
    for k in range(1, len(first)):
        total = total + first[k] * second[k]
    return total


def point_chunk(cam_ref, pt_ref, res_ref, active, at):
    def cam(side, i):
        return [cam_ref[side, i, x, :, at].astype(F32) for x in range(6)]

    pa = [[pt_ref[0, i, k, :, at].astype(F32) for k in range(3)] for i in range(2)]
    pb = [[pt_ref[1, i, k, :, at].astype(F32) for k in range(3)] for i in range(2)]
    ea = [res_ref[0, i, :, at].astype(F32) for i in range(2)]
    eb = [res_ref[1, i, :, at].astype(F32) for i in range(2)]

    def hess(m, n):
        return pa[0][m] * pa[0][n] + pa[1][m] * pa[1][n] + (pb[0][m] * pb[0][n] + pb[1][m] * pb[1][n])

    v00, v11, v22 = (hess(k, k) + POINT_DAMPING for k in range(3))
    v01, v02, v12 = hess(0, 1), hess(0, 2), hess(1, 2)
    c00 = v11 * v22 - v12 * v12
    c01 = v02 * v12 - v01 * v22
    c02 = v01 * v12 - v02 * v11
    c11 = v00 * v22 - v02 * v02
    c12 = v01 * v02 - v00 * v12
    c22 = v00 * v11 - v01 * v01
    det = v00 * c00 + v01 * c01 + v02 * c02
    scale = 1.0 / det
    i00, i01, i02 = c00 * scale, c01 * scale, c02 * scale
    i11, i12, i22 = c11 * scale, c12 * scale, c22 * scale
    inv = [[i00, i01, i02], [i01, i11, i12], [i02, i12, i22]]
    q = [-(pa[0][k] * ea[0] + pa[1][k] * ea[1] + (pb[0][k] * eb[0] + pb[1][k] * eb[1])) for k in range(3)]
    pav = [[dot3(pa[i], inv[k]) for k in range(3)] for i in range(2)]
    pbv = [[dot3(pb[i], inv[k]) for k in range(3)] for i in range(2)]

    def schur(pv, p):
        n00 = (1.0 - dot3(pv[0], p[0])) * active
        n01 = -dot3(pv[0], p[1]) * active
        n11 = (1.0 - dot3(pv[1], p[1])) * active
        return [[n00, n01], [n01, n11]]

    naa, nbb = schur(pav, pa), schur(pbv, pb)
    mab = [[-dot3(pav[i], pb[j]) * active for j in range(2)] for i in range(2)]
    ga = [-(ea[i] + dot3(pav[i], q)) * active for i in range(2)]
    gb = [-(eb[i] + dot3(pbv[i], q)) * active for i in range(2)]
    ja = [cam(0, 0), cam(0, 1)]
    jb = [cam(1, 0), cam(1, 1)]

    def quad(left, middle, right, pairs):
        half = [[middle[i][0] * right[0][y] + middle[i][1] * right[1][y] for y in range(6)] for i in range(2)]
        return [left[0][x] * half[0][y] + left[1][x] * half[1][y] for x, y in pairs]

    link = quad(ja, mab, jb, [(x, y) for x in range(6) for y in range(6)])
    diag_other = quad(jb, nbb, jb, PAIRS)
    grad_other = [jb[0][x] * gb[0] + jb[1][x] * gb[1] for x in range(6)]
    diag_own = quad(ja, naa, ja, PAIRS)
    grad_own = [ja[0][x] * ga[0] + ja[1][x] * ga[1] for x in range(6)]
    return link + diag_other + grad_other, diag_own + grad_own


def slot_sum(buffer):
    total = buffer[0]
    for k in range(1, buffer.shape[0]):
        total = total + buffer[k]
    return total


def three_terms(value):
    first = value.astype(BF16)
    rest = value - first.astype(F32)
    second = rest.astype(BF16)
    third = (rest - second.astype(F32)).astype(BF16)
    return jnp.concatenate([first.astype(F32), second.astype(F32), third.astype(F32)], axis=0)


def row_masked(stacked, which):
    line = lax.broadcasted_iota(jnp.int32, stacked.shape, 0) & 7
    return jnp.where(line == which, stacked, 0.0).astype(BF16)


def xor_flips(index, bits):
    return [(1 << k) * (1 - 2 * lax.rem(index // (1 << k), 2)) for k in range(bits)]


def flipped(index, flips, which):
    for k, flip in enumerate(flips):
        if which >> k & 1:
            index = index + flip
    return index


COL_ORDER = (11, 10, 9, 8, 7, 6, 15, 14, 3, 2, 5, 4, 13, 12, 1)
ROW_ORDER = (5, 4, 3, 7, 1, 2, 6)


def start_along(axis, me, flips, order, buffer, send, recv):
    for which in order:
        pltpu.make_async_remote_copy(
            src_ref=buffer.at[me],
            dst_ref=buffer.at[me],
            send_sem=send,
            recv_sem=recv,
            device_id={axis: flipped(me, flips, which)},
            device_id_type=MESH,
        ).start()


def wait_slots(buffer, sem):
    slots = buffer.at[pl.ds(0, buffer.shape[0] - 1)]
    pltpu.make_async_copy(slots, slots, sem).wait()


def exclusive_or(first, second, bits):
    total = 0
    for k in range(bits):
        total = total + (1 << k) * lax.rem(first // (1 << k) + second // (1 << k), 2)
    return total


def whole_kernel(
    rows, cols,
    map_hbm, count_hbm, cam_hbm, pt_hbm, res_hbm, partner_hbm, table_hbm,
    tile, update_ref, residual_ref,
    map_smem, count_smem, map_ref, cam_ref, pt_ref, res_ref, partner_ref, rank,
    high, low, own_acc, lane_index, group_index, lhs, acc, weave,
    panel, received, sums, grads, grad_parts, parts, selection,
    first_right, second_right, blocks,
    direction, remainder, answer, row_firsts, col_first, row_second, col_seconds,
    input_sems, panel_send, panel_recv, parts_send, parts_recv,
    first_send, first_recv, second_send, second_recv,
    send_row, recv_row, send_col, recv_col, send_row2, recv_row2, send_col2, recv_col2,
):
    row, col = lax.axis_index("row"), lax.axis_index("col")
    me = row * cols + col
    devices = rows * cols
    row_flips, col_flips = xor_flips(row, 3), xor_flips(col, 4)
    spread_row = functools.partial(start_along, "col", col, col_flips, COL_ORDER)
    spread_col = functools.partial(start_along, "row", row, row_flips, ROW_ORDER)
    scn, points = partner_ref.shape
    chunks = points // LANES
    lines = map_ref.shape[0]
    groups = 8

    inputs = [
        pltpu.make_async_copy(source, target, input_sems.at[k])
        for k, (source, target) in enumerate(
            (
                (map_hbm, map_smem), (count_hbm, count_smem), (table_hbm, map_ref),
                (pt_hbm, pt_ref), (cam_hbm, cam_ref), (res_hbm, res_ref), (partner_hbm, partner_ref),
            )
        )
    ]
    for copy in inputs:
        copy.start()

    barrier = pltpu.get_barrier_semaphore()

    def greet(k, carry):
        target = exclusive_or(row, k, 3)
        for j in COL_ORDER + (0,):

            def signal(column=flipped(col, col_flips, j)):
                pl.semaphore_signal(barrier, inc=1, device_id=(target, column), device_id_type=MESH)

            if j == 0:
                pl.when(k > 0)(signal)
            else:
                signal()
        return carry

    lax.fori_loop(0, rows, greet, 0)
    own_acc[...] = jnp.zeros_like(own_acc)
    acc[...] = jnp.zeros_like(acc)
    high[pl.ds((VALUES - 1) * scn, scn), :] = jnp.zeros((scn, points), F32)
    low[pl.ds((VALUES - 1) * scn, scn), :] = jnp.zeros((scn, points), F32)
    for copy in inputs:
        copy.wait()

    for s in range(scn):
        here = map_smem[me * scn + s]
        total = jnp.int32(0)
        for t in range(scn):
            if t != s:
                total = total + (map_smem[me * scn + t] < here).astype(jnp.int32)
        rank[s] = total

    def scalars_column(ref, offset, shape):
        line = lax.broadcasted_iota(jnp.int32, shape, 0)
        column = jnp.zeros(shape, jnp.int32)
        for s in range(shape[0]):
            column = jnp.where(line == s, ref[offset + s], column)
        return column

    counts = scalars_column(count_smem, 0, (scn, LANES))

    def chunk(j, carry):
        at = pl.ds(pl.multiple_of(j * LANES, LANES), LANES)
        slot = lax.broadcasted_iota(jnp.int32, (scn, LANES), 1) + j * LANES
        active = (slot < counts).astype(F32)
        values, own = point_chunk(cam_ref, pt_ref, res_ref, active, at)
        for v, value in enumerate(values):
            top = value.astype(BF16).astype(F32)
            high[pl.ds(v * scn, scn), at] = top
            low[pl.ds(v * scn, scn), at] = value - top
        for v, value in enumerate(own):
            own_acc[v] += value
        partner = partner_ref[:, at]
        which = partner & (LANES - 1)
        line = partner >> 7
        position = jnp.zeros((scn, LANES), jnp.int32)
        for h in range(lines):
            table_row = jnp.broadcast_to(map_ref[h : h + 1, :], (scn, LANES))
            position = jnp.where(line == h, jnp.take_along_axis(table_row, which, axis=1), position)
        column = position >> 7
        lane_index[:, at] = ((column >> 3) << 7) | (position & (LANES - 1))
        group_index[:, at] = column & 7
        return carry

    lax.fori_loop(0, chunks, chunk, 0)

    def scatter(s, first, count, buffer):
        group_row = jnp.broadcast_to(group_index[pl.ds(s, 1), :].astype(F32).astype(BF16), (2 * groups, points))
        group_line = lax.broadcasted_iota(jnp.int32, (2 * groups, points), 0) & (groups - 1)
        keep = group_row == group_line.astype(F32).astype(BF16)
        lane_row = lane_index[pl.ds(s, 1), :]
        onehot = jnp.where(
            lane_row == lax.broadcasted_iota(jnp.int32, (256, points), 0), 1.0, 0.0
        ).astype(BF16)
        for part, source in enumerate((high, low)):
            for v in range(0, count, 2):
                pieces = [
                    jnp.broadcast_to(source[pl.ds((first + v + k) * scn + s, 1), :], (groups, points))
                    for k in range(2)
                ]
                lhs[buffer, pl.ds((part * count + v) * groups, 2 * groups), :] = jnp.where(
                    keep, jnp.concatenate(pieces, axis=0).astype(BF16), jnp.zeros((), BF16)
                )
        result = lax.dot_general(
            lhs[buffer, : 2 * count * groups], onehot, (((1,), (1,)), ((), ())), preferred_element_type=F32
        )
        return result[: count * groups] + result[count * groups :]

    first_target = exclusive_or(row, lax.rem(col, rows), 3)

    panel_view = panel.reshape(LINK, rows, 2, 2 * groups, LANES)

    def link_rows(k, carry):
        target = exclusive_or(first_target, k, 3)
        for slot in range(2):
            s = jnp.int32(0)
            for t in range(scn):
                s = jnp.where(rank[t] == target * 2 + slot, t, s)
            result = scatter(s, 0, LINK, slot)
            for x in range(LINK):
                for b in range(2):
                    weave[pl.ds((x * 2 + b) * 2 * groups + slot, groups, stride=2), :] = result[
                        x * groups : (x + 1) * groups, b * LANES : (b + 1) * LANES
                    ]
        panel_view[:, target] = weave[...].reshape(LINK, 2, 2 * groups, LANES).astype(BF16)
        return carry

    def send_rows(k, carry):
        target = exclusive_or(first_target, k, 3)
        for j in COL_ORDER + (0,):
            column = flipped(col, col_flips, j)
            there = target * cols + column

            def send():
                pltpu.make_async_remote_copy(
                    src_ref=panel.at[:, there],
                    dst_ref=received.at[:, me],
                    send_sem=panel_send,
                    recv_sem=panel_recv,
                    device_id=(target, column),
                    device_id_type=MESH,
                ).start()

            if j == 0:
                pl.when(target != row)(send)
            else:
                send()
        return carry

    def link_and_send(k, carry):
        link_rows(k, 0)
        send_rows(k, 0)
        return carry

    link_rows(0, 0)
    pl.semaphore_wait(barrier, devices - 1)
    send_rows(0, 0)

    lanes = lax.broadcasted_iota(jnp.int32, (scn, LANES), 1)
    own_table = jnp.zeros((scn, LANES), F32)
    for v in range(DIAG + 6):
        total = jnp.sum(own_acc[v], axis=1, keepdims=True)
        own_table = jnp.where(lanes == (v if v < DIAG else GRAD_AT + v - DIAG), total, own_table)
    own_table = own_table.T[:SUM_ROWS]
    own_at = scalars_column(map_smem, me * scn, (scn, LANES))
    for column in range(2 * groups):
        spread = (own_at == lanes + column * LANES).astype(F32)
        sums[column // 2, :, (column % 2) * LANES : (column % 2 + 1) * LANES] = lax.dot_general(
            own_table, spread, (((1,), (0,)), ((), ())),
            precision=lax.Precision.HIGHEST, preferred_element_type=F32,
        )

    def other_sums(first, count):
        acc[...] = jnp.zeros_like(acc)

        def pair_sums(pair, carry):
            result = sum(scatter(pair * 2 + k, first, count, k) for k in range(2))
            for b in range(2):
                acc[pl.ds(b * (VALUES - LINK) * groups, count * groups), :] += result[
                    :, b * LANES : (b + 1) * LANES
                ]
            return carry

        lax.fori_loop(0, scn // 2, pair_sums, 0)

    def other_rows(column, count):
        return acc[pl.ds(column // groups * (VALUES - LINK) * groups + column % groups, count, stride=groups), :]

    other_sums(LINK + DIAG, 6)
    zeros = jnp.zeros((3, LANES), F32)
    for column in range(2 * groups):
        lane = slice((column % 2) * LANES, (column % 2 + 1) * LANES)
        grads[column // 2, :, lane] = sums[column // 2, GRAD_AT:, lane] + jnp.concatenate(
            [other_rows(column, 6), zeros[:2]], axis=0
        )

    def start_parts(source, target, send, recv):
        for which in ROW_ORDER:
            there = flipped(row, row_flips, which)
            pltpu.make_async_remote_copy(
                src_ref=source.at[there],
                dst_ref=target.at[row],
                send_sem=send,
                recv_sem=recv,
                device_id={"row": there},
                device_id_type=MESH,
            ).start()

    start_parts(grads, grad_parts, parts_send.at[0], parts_recv.at[0])
    grad_parts[row] = grads[row]
    lax.fori_loop(1, 4, link_and_send, 0)
    wait_slots(grad_parts, parts_recv.at[0])
    first_right[col] = slot_sum(grad_parts)
    spread_row(first_right, first_send, first_recv)
    lax.fori_loop(4, rows, link_and_send, 0)
    received[:, me] = panel[:, me]
    wait_slots(first_right, first_recv)
    second_right[row] = slot_sum(first_right)
    spread_col(second_right, second_send, second_recv)

    other_sums(LINK, DIAG + 1)
    for column in range(2 * groups):
        lane = slice((column % 2) * LANES, (column % 2 + 1) * LANES)
        sums[column // 2, :GRAD_AT, lane] += jnp.concatenate([other_rows(column, DIAG), zeros], axis=0)
    start_parts(sums.at[:, pl.ds(0, GRAD_AT)], parts, parts_send.at[1], parts_recv.at[1])
    parts[row] = sums[row, :GRAD_AT]

    offset = map_ref[...] - row * 256
    inside = (offset >= 0) & (offset < 256)
    lane = lax.broadcasted_iota(jnp.int32, (lines, LANES), 1)
    least = jnp.where(inside, offset, 256)
    for span in (1, 2, 4, 8):
        ahead = pltpu.roll(least, LANES - span, axis=1)
        behind = pltpu.roll(least, span, axis=1)
        least = jnp.minimum(least, jnp.where((lane & span) == 0, ahead, behind))
    later = (offset != least).astype(jnp.int32)
    source = (lax.broadcasted_iota(jnp.int32, (lines, LANES), 0) * 8 + (lane >> 4)) * 2 + later
    place = jnp.where(inside, offset, -1)
    source = jnp.where(inside, source, -1)
    deep = lax.broadcasted_iota(jnp.int32, (256, LANES), 0)
    chosen = jnp.zeros((256, 256), F32)
    for h in range(lines):
        place_hot = jnp.where(place[h : h + 1] == deep, 1.0, 0.0).astype(BF16)
        source_hot = jnp.where(source[h : h + 1] == deep, 1.0, 0.0).astype(BF16)
        chosen = chosen + lax.dot_general(
            place_hot, source_hot, (((1,), (1,)), ((), ())), preferred_element_type=F32
        )
    selection[...] = chosen.astype(BF16)

    landed = received.at[:, pl.ds(0, devices - 1)]
    pltpu.make_async_copy(landed, landed, panel_recv).wait()
    received_view = received.reshape(LINK, 2 * devices, LANES)

    def select(block, carry):
        for k in range(6):
            x = (block * 6 + k) * 2
            pair = jnp.concatenate([received_view[x], received_view[x + 1]], axis=1)
            chosen_rows = jnp.dot(selection[...], pair, preferred_element_type=F32).astype(BF16)
            tile[x] = chosen_rows[:, :LANES]
            tile[x + 1] = chosen_rows[:, LANES:]
        return carry

    lax.fori_loop(0, LINK // 12, select, 0)

    wait_slots(second_right, second_recv)
    start = second_right[...]
    direction[...] = start
    remainder[...] = start
    answer[...] = jnp.zeros_like(answer)

    def inner_product(first, second):
        total = first[0] * second[0]
        for r in range(1, rows):
            total = total + first[r] * second[r]
        return jnp.sum(jnp.sum(total, axis=0, keepdims=True), axis=1, keepdims=True)

    norm_start = inner_product(start, start)
    wait_slots(parts, parts_recv.at[1])
    total = slot_sum(parts)
    line = lax.broadcasted_iota(jnp.int32, (8, 256), 0)
    for y in range(6):
        block = jnp.zeros((8, 256), F32)
        for x in range(6):
            v = pair_index(x, y)
            block = jnp.where(line == x, jnp.broadcast_to(total[v : v + 1], (8, 256)), block)
        blocks[y] = block

    def iteration(step, norm_now):
        parity = lax.rem(step, 2)
        row_first, col_second = row_firsts.at[parity], col_seconds.at[parity]
        rows_part = direction[row]
        cols_part = direction[col // 2, :, pl.ds(pl.multiple_of(lax.rem(col, 2) * LANES, LANES), LANES)]
        row_terms, col_terms = three_terms(rows_part), three_terms(cols_part)
        col_lhs = [row_masked(col_terms, y) for y in range(6)]
        row_lhs = [row_masked(row_terms, x) for x in range(6)]
        line_rows = lax.broadcasted_iota(jnp.int32, (8, 256), 0)
        line_cols = lax.broadcasted_iota(jnp.int32, (8, LANES), 0)
        forward = jnp.zeros((8, 256), F32)
        for y in range(6):
            forward = forward + blocks[y] * jnp.broadcast_to(rows_part[y : y + 1], (8, 256))
        for x in range(6):
            wide = jnp.concatenate([tile[x * 6 + y] for y in range(6)], axis=1)
            total = lax.dot_general(
                jnp.concatenate(col_lhs, axis=1), wide, (((1,), (1,)), ((), ())), preferred_element_type=F32
            )
            forward = forward + jnp.where(line_rows == x, jnp.sum(total, axis=0, keepdims=True), 0.0)
        row_first[col] = forward
        spread_row(row_first, send_row.at[parity], recv_row.at[parity])
        backward = jnp.zeros((8, LANES), F32)
        for y in range(6):
            total = None
            for x in range(6):
                part = jnp.dot(row_lhs[x], tile[x * 6 + y], preferred_element_type=F32)
                total = part if total is None else total + part
            backward = backward + jnp.where(line_cols == y, jnp.sum(total, axis=0, keepdims=True), 0.0)
        col_first[row] = backward
        spread_col(col_first, send_col, recv_col)
        wait_slots(col_first, recv_col)
        col_second[col] = slot_sum(col_first)
        spread_row(col_second, send_col2.at[parity], recv_col2.at[parity])
        wait_slots(row_first, recv_row.at[parity])
        row_second[row] = slot_sum(row_first)
        spread_col(row_second, send_row2, recv_row2)
        wait_slots(row_second, recv_row2)
        wait_slots(col_second, recv_col2.at[parity])
        wait_slots(row_first, send_row.at[parity])
        wait_slots(col_first, send_col)
        wait_slots(row_second, send_row2)
        wait_slots(col_second, send_col2.at[parity])
        held = direction[...]
        image = CAMERA_DAMPING * held + row_second[...]
        back = jnp.stack(
            [jnp.concatenate([col_second[2 * r], col_second[2 * r + 1]], axis=1) for r in range(rows)], axis=0
        )
        image = image + back
        step_size = norm_now / inner_product(held, image)
        answer[...] = answer[...] + step_size[None] * held
        left = remainder[...] - step_size[None] * image
        remainder[...] = left
        norm_next = inner_product(left, left)
        direction[...] = left + (norm_next / norm_now)[None] * held
        return norm_next

    lax.fori_loop(0, ITERS, iteration, norm_start)
    update_ref[...] = answer[row][:6]
    residual_ref[...] = remainder[row][:6]
    sent = panel.at[:, pl.ds(0, devices - 1)]
    pltpu.make_async_copy(sent, sent, panel_send).wait()
    wait_slots(grad_parts, parts_send.at[0])
    wait_slots(parts, parts_send.at[1])
    wait_slots(first_right, first_send)
    wait_slots(second_right, second_send)


def store_kernel(*refs):
    count = len(refs) // 2
    sems = refs[-1]
    copies = [pltpu.make_async_copy(refs[k], refs[count + k], sems.at[k]) for k in range(count)]
    for copy in copies:
        copy.start()
    for copy in copies:
        copy.wait()


def store(arrays):
    return pl.pallas_call(
        store_kernel,
        in_specs=[pl.BlockSpec(memory_space=pltpu.VMEM)] * len(arrays),
        out_specs=[pl.BlockSpec(memory_space=pltpu.HBM)] * len(arrays),
        out_shape=[jax.ShapeDtypeStruct(array.shape, array.dtype) for array in arrays],
        scratch_shapes=[pltpu.SemaphoreType.DMA((len(arrays),))],
        compiler_params=pltpu.CompilerParams(vmem_limit_bytes=8 * 1024 * 1024),
        name="store",
    )(*arrays)


def shards(cam_jac, pt_jac, resid, partner, count, tile_map):
    rows, cols = lax.axis_size("row"), lax.axis_size("col")
    scn, points = partner.shape
    devices = rows * cols
    groups = 8
    dma = pltpu.SemaphoreType.DMA
    vmem = pltpu.VMEM
    vmem_spec = pl.BlockSpec(memory_space=pltpu.VMEM)
    hbm_spec = pl.BlockSpec(memory_space=pltpu.HBM)
    coupling, update, residual = pl.pallas_call(
        functools.partial(whole_kernel, rows, cols),
        in_specs=[hbm_spec] * 7,
        out_specs=[vmem_spec] * 3,
        out_shape=[
            jax.ShapeDtypeStruct((LINK, 256, LANES), BF16),
            jax.ShapeDtypeStruct((6, 256), F32),
            jax.ShapeDtypeStruct((6, 256), F32),
        ],
        scratch_shapes=[
            pltpu.SMEM(tile_map.shape, jnp.int32),
            pltpu.SMEM(count.shape, jnp.int32),
            vmem((tile_map.shape[0] // LANES, LANES), jnp.int32),
            vmem(cam_jac.shape, BF16),
            vmem(pt_jac.shape, BF16),
            vmem(resid.shape, BF16),
            vmem(partner.shape, jnp.int32),
            pltpu.SMEM((scn,), jnp.int32),
            vmem((VALUES * scn, points), F32),
            vmem((VALUES * scn, points), F32),
            vmem((DIAG + 6, scn, LANES), F32),
            vmem((scn, points), jnp.int32),
            vmem((scn, points), jnp.int32),
            vmem((2, 2 * LINK * groups, points), BF16),
            vmem((2 * (VALUES - LINK) * groups, LANES), F32),
            vmem((LINK * 2 * 2 * groups, LANES), F32),
            vmem((LINK, devices, 2, LANES), BF16),
            vmem((LINK, devices, 2, LANES), BF16),
            vmem((rows, SUM_ROWS, 256), F32),
            vmem((rows, 8, 256), F32),
            vmem((rows, 8, 256), F32),
            vmem((rows, GRAD_AT, 256), F32),
            vmem((256, 256), BF16),
            vmem((cols, 8, 256), F32),
            vmem((rows, 8, 256), F32),
            vmem((6, 8, 256), F32),
            vmem((rows, 8, 256), F32),
            vmem((rows, 8, 256), F32),
            vmem((rows, 8, 256), F32),
            vmem((2, cols, 8, 256), F32),
            vmem((rows, 8, LANES), F32),
            vmem((rows, 8, 256), F32),
            vmem((2, cols, 8, LANES), F32),
            dma((7,)), dma, dma, dma((2,)), dma((2,)),
            dma, dma, dma, dma,
            dma((2,)), dma((2,)), dma, dma, dma, dma, dma((2,)), dma((2,)),
        ],
        compiler_params=pltpu.CompilerParams(
            collective_id=0, has_side_effects=True, vmem_limit_bytes=48 * 1024 * 1024
        ),
        name="bundle",
    )(
        *(
            pltpu.with_memory_space_constraint(array, pltpu.HBM)
            for array in (tile_map, count, cam_jac, pt_jac, resid, partner, tile_map.reshape(-1, LANES))
        )
    )
    coupling, update, residual = store([coupling, update, residual])
    return coupling.reshape(6, 6, 256, LANES), update, residual


def solution(mesh):
    return jax.shard_map(
        shards,
        mesh=mesh,
        in_specs=(
            P(None, None, None, ("row", "col"), None),
            P(None, None, None, ("row", "col"), None),
            P(None, None, ("row", "col"), None),
            P(("row", "col"), None),
            P(("row", "col")),
            P(),
        ),
        out_specs=(P(None, None, "row", "col"), P(None, "row"), P(None, "row")),
        check_vma=False,
    )
```
